256 devices in a mesh: groups: 2 (over z), seq: 64 (over y, x), expert: 2 (over core).
Axes of the slice: x: 8, y: 8, z: 2, core: 2. Of those that a mesh axis runs over, the one named last changes fastest.
The devices are a block of a 8x8x16 slice.
Arguments:
- residual: bfloat16 [8, 6144], P('groups', 'seq'), parts along dimension 0, may hold values from -27 to 27
- queries: bfloat16 [8, 6144], P('groups', 'expert'), parts along dimension 0, may hold values from -6 to 6
- new_entries: bfloat16 [2, 8, 1024], P(None, 'groups', 'expert'), parts along dimension 1, may hold values from -6 to 6
- kv_cache: bfloat16 [2, 1024, 131072], P(None, 'seq', ('groups', 'expert')), parts along dimension 2, may hold values from -6 to 6
- lengths: int32 [8], P('groups'), parts along dimension 0, may hold values from 1024 to 16384, as said below
- routing: int32 [8, 2], P('groups'), parts along dimension 0, may hold values from 0 to 3, all different within a row
- w_out: bfloat16 [6144, 6144], P('expert', 'seq'), may hold values from -0.5 to 0.5
- norm_gain: bfloat16 [6144], replicated, may hold values from 0.5 to 1.5
- router: bfloat16 [6144, 4], replicated, may hold values from -0.078125 to 0.078125
- w_gate: bfloat16 [4, 6144, 8192], P('expert', None, 'seq'), may hold values from -0.078125 to 0.078125
- w_up: bfloat16 [4, 6144, 8192], P('expert', None, 'seq'), may hold values from -0.078125 to 0.078125
- w_down: bfloat16 [4, 8192, 6144], P('expert', 'seq'), may hold values from -0.5 to 0.5
Outputs:
- attended: bfloat16 [8, 6144], P('groups', 'seq'), parts along dimension 0
- expert_out: bfloat16 [8, 6144], P('groups', 'seq'), parts along dimension 0
The draws below stay inside these ranges and needn't reach their ends.
There are 2 independent parts, one for each index of `groups`. The reference program is written for one: setup_inputs(seed, part) draws one part's arguments, and reference() takes and returns one part's arrays. A program takes and returns all parts, laid end to end along the dimension named above; an argument that names none is the same for every part. Nothing has to cross between parts.
Inputs may be any that keep to these rules, and one draw needn't show every extreme that they name: `lengths`: every draw has a request of exactly 16384 positions. `routing`: each request names two different experts.
All inputs are finite; a program needn't handle non-finite values.
Results may differ from the reference program's by a relative error of at most 0.02.
Values may be sent and summed in bfloat16 or wider, within the bound.
No kernel may reach another device: no remote copies, remote signals or barrier semaphores. Data moves between devices by JAX's collectives and lax.ppermute only.
A program may use at most 128 MiB of HBM per device.

```python
import math
import jax
import jax.numpy as jnp
from jax import lax

D = 6144
H = 48
KVH = 8
HD = 128
EXPERTS = 4
FF = 8192
REQ = 4
CTX = 16384


def draw_residual(key, part):
    drawn = 0.5 * jnp.clip(jax.random.normal(jax.random.fold_in(key, 1), (REQ, D), jnp.float32), -6.0, 6.0)
    return drawn.astype(jnp.bfloat16)


def draw_queries(key, part):
    drawn = jnp.clip(jax.random.normal(jax.random.fold_in(key, 4), (REQ, H * HD), jnp.float32), -6.0, 6.0)
    return drawn.astype(jnp.bfloat16)


def draw_new_entries(key, part):
    drawn = jnp.clip(jax.random.normal(jax.random.fold_in(key, 5), (2, REQ, KVH * HD), jnp.float32), -6.0, 6.0)
    return drawn.astype(jnp.bfloat16)


def draw_kv_cache(key, part):
    drawn = jnp.clip(jax.random.normal(jax.random.fold_in(key, 6), (2, KVH * HD, CTX * REQ), jnp.float32), -6.0, 6.0)
    return drawn.astype(jnp.bfloat16)


def draw_lengths(key, part):
    drawn = jax.random.randint(jax.random.fold_in(key, 11), (REQ,), CTX // 16, CTX + 1, dtype=jnp.int32)
    longest = jax.random.randint(jax.random.fold_in(key, 12), (), 0, REQ, dtype=jnp.int32)
    return jnp.where(jnp.arange(REQ, dtype=jnp.int32) == longest, CTX, drawn).astype(jnp.int32)


def spiked(values, key, source, target, shards_of, factor):
    def block_of(position):
        return (jnp.arange(values.shape[position]) // (values.shape[position] // shards_of)).reshape((-1,) + (1,) * (values.ndim - 1 - position))

    first = jax.random.permutation(key, shards_of)[block_of(target)]
    other_side = (block_of(target) + shards_of // 2) % shards_of
    return jnp.where((block_of(source) == first) | (block_of(source) == other_side), factor * values, values)


def block_levels(key, dims, split, least, largest):
    loudness = 1.0
    for position, parts in split:
        steps = jax.random.uniform(jax.random.fold_in(jax.random.fold_in(key, 6), position), (parts,), jnp.float32, least / len(split), largest / len(split))
        loudness = loudness * jnp.repeat(jnp.exp(steps), dims[position] // parts).reshape((-1,) + (1,) * (len(dims) - 1 - position))
    return loudness


def picks_of(own_key, rows, count, top, lift):
    ranking = jax.random.permutation(jax.random.fold_in(own_key, 1), count)
    pull = ranking
    for power in range(3):
        pull = pull * pull // count
    pull = pull * lift // count
    chance = jax.random.randint(jax.random.fold_in(own_key, 2), (rows, count), 0, 4096) + pull
    fixed_rows = jax.random.permutation(jax.random.fold_in(own_key, 3), rows)[jnp.arange(count) % rows]
    chance = jnp.where(jnp.arange(rows)[:, None] == fixed_rows[None, :], 1 << 14, chance)
    score = chance * count + jnp.arange(count)
    return lax.top_k(score.astype(jnp.int32), top)[1].astype(jnp.int32)


def gaussian(stream_key, shape, width, most, cuts=(), kind=jnp.bfloat16):
    values = width * jax.random.normal(stream_key, shape, jnp.float32)
    if cuts:
        values = values * block_levels(stream_key, shape, cuts, -0.22, 0.18)
    return jnp.clip(values, -most, most).astype(kind)


def gaussian_with(rng, extent, width, most, pieces, heavy, held_as=jnp.bfloat16):
    values = width * jax.random.normal(rng, extent, jnp.float32)
    if pieces:
        values = values * block_levels(rng, extent, pieces, -0.22, 0.18)
    return jnp.clip(spiked(values, jax.random.fold_in(rng, 3), *heavy), -most, most).astype(held_as)


def setup_inputs(seed: int = 0, part: int = 0) -> dict:
    seeds = jax.random.split(jax.random.key(seed), 13)
    part_keys = jax.random.split(jax.random.fold_in(seeds[12], part), 13)
    return {
        "residual": draw_residual(jax.random.fold_in(jax.random.fold_in(seeds[12], part), 71), part),
        "queries": draw_queries(jax.random.fold_in(jax.random.fold_in(seeds[12], part), 71), part),
        "new_entries": draw_new_entries(jax.random.fold_in(jax.random.fold_in(seeds[12], part), 71), part),
        "kv_cache": draw_kv_cache(jax.random.fold_in(jax.random.fold_in(seeds[12], part), 71), part),
        "lengths": draw_lengths(jax.random.fold_in(jax.random.fold_in(seeds[12], part), 71), part),
        "routing": picks_of(part_keys[5], REQ, EXPERTS, 2, 4096),
        "w_out": gaussian(seeds[6], (H * HD, D), HD ** -0.5, 0.5, ((0, 2), (1, 64))),
        "norm_gain": jnp.clip(1.0 + 0.1 * jax.random.normal(seeds[7], (D,), jnp.float32), 0.5, 1.5).astype(jnp.bfloat16),
        "router": gaussian(seeds[8], (D, EXPERTS), D ** -0.5, 0.078125),
        "w_gate": gaussian(seeds[9], (EXPERTS, D, FF), D ** -0.5, 0.078125, ((0, 2), (2, 64))),
        "w_up": gaussian(seeds[10], (EXPERTS, D, FF), D ** -0.5, 0.078125, ((0, 2), (2, 64))),
        "w_down": gaussian_with(seeds[11], (EXPERTS, FF, D), (FF // 8) ** -0.5, 0.5, ((0, 2), (1, 64)), (1, 2, 64, 4.0)),
    }


def reference(residual, queries, new_entries, kv_cache, lengths, routing, w_out, norm_gain, router, w_gate, w_up, w_down):
    per_group = H // KVH
    score_scale = 1.0 / math.sqrt(HD)
    key_rows = kv_cache[0].reshape(KVH, HD, CTX, REQ).astype(jnp.float32)
    value_rows = kv_cache[1].reshape(KVH, HD, CTX, REQ).astype(jnp.float32)
    query_heads = queries.reshape(REQ, KVH, per_group, HD).astype(jnp.float32)
    new_keys = new_entries[0].reshape(REQ, KVH, HD).astype(jnp.float32)
    new_values = new_entries[1].reshape(REQ, KVH, HD).astype(jnp.float32)
    scores = jnp.einsum('rgtd,gdpr->rgtp', query_heads, key_rows, precision=lax.Precision.HIGHEST) * score_scale
    own_score = jnp.einsum('rgtd,rgd->rgt', query_heads, new_keys, precision=lax.Precision.HIGHEST) * score_scale
    alive_mask = (jnp.arange(CTX, dtype=jnp.int32)[None, :] < lengths[:, None])[:, None, None, :]
    highest = jnp.maximum(lax.optimization_barrier(jnp.max(jnp.where(alive_mask, scores, -1e+30), axis=-1)), own_score)
    weights = jnp.where(alive_mask, jnp.exp(scores - highest[..., None]), 0.0)
    own_weight = jnp.exp(own_score - highest)
    totals = lax.optimization_barrier(jnp.sum(weights, axis=-1)) + own_weight
    rounded = lax.optimization_barrier(weights.astype(jnp.bfloat16)).astype(jnp.float32)
    summed = jnp.einsum('rgtp,gdpr->rgtd', rounded, value_rows, precision=lax.Precision.HIGHEST)
    summed = summed + own_weight[..., None] * new_values[:, :, None, :]
    attn_rows = (summed / totals[..., None]).reshape(REQ, H * HD).astype(jnp.bfloat16)
    attended = (residual.astype(jnp.float32) + jnp.dot(attn_rows, w_out, preferred_element_type=jnp.float32)).astype(jnp.bfloat16)
    widened = attended.astype(jnp.float32)
    mean_square = lax.optimization_barrier(jnp.mean(widened * widened, axis=-1, keepdims=True))
    normed = (widened * lax.rsqrt(mean_square + 1e-05) * norm_gain.astype(jnp.float32)).astype(jnp.bfloat16)
    logits = jnp.dot(normed, router, preferred_element_type=jnp.float32)
    picked = (routing[:, :, None] == jnp.arange(EXPERTS, dtype=jnp.int32)[None, None, :]).astype(jnp.float32)
    chosen = lax.optimization_barrier(jnp.sum(picked * logits[:, None, :], axis=-1))
    first_share = jax.nn.sigmoid(chosen[:, 0] - chosen[:, 1])
    shares = jnp.stack([first_share, 1.0 - first_share], axis=-1)
    combine = lax.optimization_barrier(jnp.sum(picked * shares[:, :, None], axis=1))

    def one_expert(expert):
        gate_proj = jnp.dot(normed, w_gate[expert], preferred_element_type=jnp.float32)
        upward = jnp.dot(normed, w_up[expert], preferred_element_type=jnp.float32)
        weight_col = lax.dynamic_slice_in_dim(combine, expert, 1, 1)
        activation = (jax.nn.silu(gate_proj) * upward * weight_col).astype(jnp.bfloat16)
        return jnp.dot(activation, w_down[expert], preferred_element_type=jnp.float32)
    expert_terms = lax.map(one_expert, jnp.arange(EXPERTS, dtype=jnp.int32))
    expert_out = lax.optimization_barrier(jnp.sum(expert_terms, axis=0)).astype(jnp.bfloat16)
    return (attended, expert_out)
```

```python
import math

import jax
import jax.numpy as jnp
from jax import lax
from jax.experimental import pallas as pl
from jax.experimental.pallas import tpu as pltpu
from jax.sharding import Mesh
from jax.sharding import PartitionSpec as P

H = 48
KVH = 8
HD = 128
PER = H // KVH
Y = "seq_0"
X = "seq_1"
SEQ = (Y, X)
E = "expert"
LANES = 128
ROWS = 8
FOLD = 4
HEADS = 4
F32 = jnp.float32
BF16 = jnp.bfloat16
LOW = -1e30
LARGEST = 6.0
SCALE = 1.0 / math.sqrt(HD)
PARAMS = pltpu.CompilerParams(vmem_limit_bytes=16 << 20)
NT = (((1,), (1,)), ((), ()))
NN = (((1,), (0,)), ((), ()))


def iota(shape, dim):
    return lax.broadcasted_iota(jnp.int32, shape, dim)


def vmem():
    return pl.BlockSpec(memory_space=pltpu.VMEM)


def exponent_per_unit(depth):
    return 80.0 / (LARGEST * LARGEST * depth * SCALE)


def near(array):
    return pltpu.with_memory_space_constraint(array, pltpu.VMEM)


def far(array):
    return pltpu.with_memory_space_constraint(array, pltpu.HBM)


def swapped(shard):
    return lax.ppermute(shard, E, [(0, 1), (1, 0)])


def to_everyone(copies, axes):
    return lax.all_to_all(copies, axes, split_axis=0, concat_axis=0, tiled=True)


def pack_kernel(q_ref, new_ref, lengths_ref, packed_ref, limit_ref, sizes_ref, sems):
    requests = q_ref.shape[0]
    own_heads = q_ref.shape[1] // (PER * HD)
    local = lax.axis_index(Y) % own_heads
    span = PER * HD
    head = pl.ds(pl.multiple_of(local * HD, LANES), HD)
    copies = [
        pltpu.make_async_copy(lengths_ref, sizes_ref, sems.at[0]),
        pltpu.make_async_copy(
            q_ref.at[:, pl.ds(pl.multiple_of(local * span, LANES), span)], packed_ref.at[:, 0:span], sems.at[1]
        ),
    ]
    for i in range(2):
        copies.append(
            pltpu.make_async_copy(
                new_ref.at[i, :, head], packed_ref.at[:, span + i * HD : span + (i + 1) * HD], sems.at[2 + i]
            )
        )
    for copy in copies:
        copy.start()
    copies[0].wait()
    which = iota((ROWS, LANES), 1) % requests
    limit = jnp.full((ROWS, LANES), sizes_ref[0], jnp.int32)
    for r in range(1, requests):
        limit = jnp.where(which == r, sizes_ref[r], limit)
    limit_ref[...] = limit
    for copy in copies[1:]:
        copy.wait()


def packed(queries, new_entries, lengths):
    requests = queries.shape[0]
    return pl.pallas_call(
        pack_kernel,
        in_specs=[pl.BlockSpec(memory_space=pltpu.HBM)] * 3,
        out_specs=[vmem()] * 2,
        out_shape=[
            pltpu.VMEM((requests, PER * HD + 2 * HD), BF16),
            pltpu.VMEM((ROWS, LANES), jnp.int32),
        ],
        scratch_shapes=[pltpu.SMEM((requests,), jnp.int32), pltpu.SemaphoreType.DMA((4,))],
        compiler_params=PARAMS,
        name="pack",
    )(far(queries), far(new_entries), far(lengths))


def score_kernel(peers, own_heads, mine_ref, other_ref, k_ref, kv_ref, s_ref, own_ref, v_ref, rows_ref, sem):
    requests = mine_ref.shape[0]
    depth = k_ref.shape[0]
    width = k_ref.shape[1] // peers
    slim = width // FOLD
    fetch = pltpu.make_async_copy(kv_ref.at[1], v_ref, sem)
    fetch.start()
    x = lax.axis_index(X)
    mine = (lax.axis_index(Y) // own_heads) == lax.axis_index(E)
    q = jnp.where(mine, mine_ref[...].astype(F32), other_ref[...].astype(F32))
    rows_ref[...] = jnp.zeros_like(rows_ref)
    for r in range(requests):
        for t in range(PER):
            rows_ref[r * ROWS + t : r * ROWS + t + 1, :] = q[r : r + 1, t * HD : (t + 1) * HD]
    fresh = [q[:, (PER + i) * HD : (PER + i + 1) * HD].astype(BF16) for i in range(2)]

    rolled = pltpu.roll(rows_ref[0 : requests * ROWS, :], (HD - x * depth) % HD, 1)
    query = rolled[:, 0:depth].astype(BF16)
    which = iota((ROWS, slim), 1) % requests
    for c in range(peers):
        folds = []
        for k in range(FOLD):
            at = c * width + k * slim
            found = lax.dot_general(query, k_ref[:, at : at + slim], NN, preferred_element_type=F32)
            score = found[0:ROWS]
            for r in range(1, requests):
                score = jnp.where(which == r, found[r * ROWS : (r + 1) * ROWS], score)
            folds.append(score[0:PER])
        power = jnp.concatenate(folds, axis=0) * (SCALE * exponent_per_unit(depth))
        s_ref[c] = jnp.exp(power).astype(BF16)

    rows = rows_ref[...].astype(BF16)
    every = lax.dot_general(fresh[0], rows, NT, preferred_element_type=F32)
    own_row = iota(every.shape, 1) // ROWS == iota(every.shape, 0)
    score = jnp.sum(jnp.where(own_row, every, 0.0), axis=0, keepdims=True) * SCALE
    pick = (iota((depth, HD), 1) == iota((depth, HD), 0) + x * depth).astype(BF16)
    values = lax.dot_general(pick, fresh[1], NT, preferred_element_type=F32).astype(BF16)
    spread = (iota((requests, LANES), 1) // ROWS == iota((requests, LANES), 0)).astype(BF16)
    own_ref[0:depth, :] = lax.dot_general(values, spread, NN, preferred_element_type=F32)
    line = iota((ROWS, LANES), 0)
    own_ref[depth : depth + ROWS, :] = jnp.where(line == 0, 1.0, jnp.where(line == 1, score, 0.0))
    fetch.wait()


def key_kernel(kv_ref, k_ref, sem):
    fetch = pltpu.make_async_copy(kv_ref.at[0], k_ref, sem)
    fetch.start()
    fetch.wait()


def fetched_keys(kv_cache):
    return pl.pallas_call(
        key_kernel,
        in_specs=[pl.BlockSpec(memory_space=pltpu.HBM)],
        out_specs=vmem(),
        out_shape=pltpu.VMEM(kv_cache.shape[1:], BF16),
        scratch_shapes=[pltpu.SemaphoreType.DMA],
        compiler_params=PARAMS,
        name="keys",
    )(far(kv_cache))


def partial_scores(mine, other, keys, kv_cache):
    depth = kv_cache.shape[1]
    peers = lax.axis_size(X)
    own_heads = KVH // lax.axis_size(E)
    slim = kv_cache.shape[2] // peers // FOLD
    return pl.pallas_call(
        lambda *refs: score_kernel(peers, own_heads, *refs),
        in_specs=[vmem()] * 3 + [pl.BlockSpec(memory_space=pltpu.HBM)],
        out_specs=[vmem()] * 3,
        out_shape=[
            pltpu.VMEM((peers, FOLD * PER, slim), BF16),
            pltpu.VMEM((depth + ROWS, LANES), F32),
            pltpu.VMEM(kv_cache.shape[1:], BF16),
        ],
        scratch_shapes=[pltpu.VMEM((LANES, HD), F32), pltpu.SemaphoreType.DMA],
        compiler_params=PARAMS,
        name="scores",
    )(near(mine), near(other), near(keys), far(kv_cache))


def weight_kernel(requests, half_ctx, parts_ref, limit_ref, w_ref):
    peers, tall, slim = parts_ref.shape
    blocks = slim // LANES
    start = lax.axis_index(E) * half_ctx + lax.axis_index(X) * (FOLD * slim // requests)
    limit = jnp.concatenate([limit_ref[...]] * (tall // ROWS), axis=0)
    place = iota((tall, LANES), 1) // requests + start + (iota((tall, LANES), 0) // PER) * (slim // requests)
    scores = []
    high = jnp.full((tall, LANES), LOW, F32)
    for j in range(blocks):
        at = slice(j * LANES, (j + 1) * LANES)
        total = jnp.log(parts_ref[0, :, at].astype(F32))
        for c in range(1, peers):
            total = total + jnp.log(parts_ref[c, :, at].astype(F32))
        alive = place + j * (LANES // requests) < limit
        total = jnp.where(alive, total * (1.0 / exponent_per_unit(HD // peers)), LOW)
        scores.append(total)
        high = jnp.maximum(high, total)
    best = high[0:PER]
    for k in range(1, FOLD):
        best = jnp.maximum(best, high[k * PER : (k + 1) * PER])
    step = requests
    while step < LANES:
        best = jnp.maximum(best, pltpu.roll(best, step, 1))
        step *= 2
    best16 = best.astype(BF16)
    best = best16.astype(F32)
    high = jnp.concatenate([best] * FOLD, axis=0)
    shown = jnp.concatenate([best, jnp.zeros((ROWS - PER, LANES), F32)], axis=0).astype(BF16)
    groups = tall // ROWS
    for j in range(blocks):
        alive = place + j * (LANES // requests) < limit
        weight = jnp.where(alive, jnp.exp(scores[j] - high), 0.0)
        for i in range(groups):
            tile = weight[i * ROWS : (i + 1) * ROWS].astype(BF16)
            for c in range(peers):
                w_ref[c, j * groups + i] = tile
    for c in range(peers):
        w_ref[c, blocks * groups] = shown


def local_weights(parts, limit, requests, half_ctx):
    peers, tall, slim = parts.shape
    tiles = (tall // ROWS) * (slim // LANES) + 1
    return pl.pallas_call(
        lambda *refs: weight_kernel(requests, half_ctx, *refs),
        in_specs=[vmem()] * 2,
        out_specs=vmem(),
        out_shape=pltpu.VMEM((peers, tiles, ROWS, LANES), BF16),
        compiler_params=PARAMS,
        name="weights",
    )(near(parts), near(limit))


def value_kernel(requests, w_ref, v_ref, out_ref):
    peers, tiles = w_ref.shape[:2]
    depth = v_ref.shape[0]
    slim = v_ref.shape[1] // peers // FOLD
    blocks = slim // LANES
    groups = (tiles - 1) // blocks
    used = requests * ROWS
    tops = [w_ref[c, tiles - 1].astype(F32) for c in range(peers)]
    best = tops[0]
    for c in range(1, peers):
        best = jnp.maximum(best, tops[c])
    which = iota((ROWS, slim), 1) % requests
    spare = jnp.zeros((ROWS - PER, slim), F32)
    ones = jnp.ones((depth, slim), BF16)
    acc = jnp.zeros((2 * depth, used), F32)
    for c in range(peers):
        fade = jnp.concatenate([jnp.exp(tops[c] - best)[0:PER]] * FOLD, axis=0)
        weight = jnp.concatenate(
            [
                jnp.concatenate([w_ref[c, j * groups + i].astype(F32) for i in range(groups)], axis=0) * fade
                for j in range(blocks)
            ],
            axis=1,
        )
        for k in range(FOLD):
            part = jnp.concatenate([weight[k * PER : (k + 1) * PER], spare], axis=0)
            masked = jnp.concatenate([jnp.where(which == r, part, 0.0) for r in range(requests)], axis=0)
            at = (c * FOLD + k) * slim
            values = jnp.concatenate([v_ref[:, at : at + slim], ones], axis=0)
            acc = acc + lax.dot_general(values, masked.astype(BF16), NT, preferred_element_type=F32)
    lane = iota((ROWS, LANES), 1)
    line = iota((ROWS, LANES), 0)
    mixed = jnp.where((lane // requests == line) & (lane < used), best, 0.0)
    row = jnp.broadcast_to(jnp.sum(mixed, axis=0, keepdims=True), (ROWS, LANES)).astype(BF16)
    a, b = iota((LANES, LANES), 0), iota((LANES, LANES), 1)
    moved = ((a // requests == b % ROWS) & (a % requests == b // ROWS)).astype(BF16)
    top = lax.dot_general(row, moved, NN, preferred_element_type=F32)
    out_ref[...] = jnp.zeros_like(out_ref)
    out_ref[0 : depth + ROWS, 0:used] = acc[0 : depth + ROWS]
    out_ref[depth : depth + ROWS, :] = jnp.where(line == 1, top, out_ref[depth : depth + ROWS, :])


def weighted_values(weights, values, requests):
    depth = values.shape[0]
    return pl.pallas_call(
        lambda *refs: value_kernel(requests, *refs),
        in_specs=[vmem()] * 2,
        out_specs=vmem(),
        out_shape=pltpu.VMEM((depth + ROWS, LANES), F32),
        compiler_params=PARAMS,
        name="values",
    )(near(weights), near(values))


def merge_kernel(own_ref, left_ref, right_ref, out_ref):
    depth = own_ref.shape[0] - ROWS
    parts = (own_ref, left_ref, right_ref)
    highs = [p[depth + 1 : depth + 2, :] for p in parts]
    high = jnp.maximum(jnp.maximum(highs[0], highs[1]), highs[2])
    total = jnp.zeros((1, LANES), F32)
    summed = jnp.zeros((depth, LANES), F32)
    for part, top in zip(parts, highs):
        fade = jnp.exp(top - high)
        total = total + part[depth : depth + 1, :] * fade
        summed = summed + part[0:depth, :] * fade
    attn = summed / total
    held = jnp.zeros((ROWS, LANES), F32)
    for b in range(depth // ROWS):
        held = held + pltpu.roll(attn[b * ROWS : (b + 1) * ROWS], b * (LANES // HEADS), 1)
    held = held.astype(BF16)
    for k in range(out_ref.shape[0]):
        out_ref[k] = held


def merged(own, left, right, copies):
    return pl.pallas_call(
        merge_kernel,
        in_specs=[vmem()] * 3,
        out_specs=vmem(),
        out_shape=pltpu.VMEM((copies, ROWS, LANES), BF16),
        compiler_params=PARAMS,
        name="merge",
    )(near(own), near(left), near(right))


def project_kernel(requests, attn_ref, w_ref, out_ref):
    width = w_ref.shape[0]
    heads = w_ref.shape[1] // (PER * HD)
    along = attn_ref.shape[0] // KVH
    blocks = HD // along // ROWS
    part = LANES // HEADS
    start = lax.axis_index(E) * (heads * along)
    pieces = [
        attn_ref[pl.ds(start + g * along, along)].astype(F32).reshape(along * ROWS, LANES) for g in range(heads)
    ]
    group = iota((along * ROWS, LANES), 1) // part
    stacked = []
    for b in range(blocks):
        mixed = jnp.zeros((along * ROWS, LANES), F32)
        for g in range(heads):
            mixed = jnp.where(group == g, pltpu.roll(pieces[g], ((g - b) * part) % LANES, 1), mixed)
        stacked.append(mixed)
    mixed = jnp.concatenate(stacked, axis=0).astype(BF16)
    d, k = iota((HD, HD), 0), iota((HD, HD), 1)
    order = (
        (d // (blocks * ROWS) == (k // ROWS) % along)
        & ((d // ROWS) % blocks == k // (along * ROWS))
        & (d % ROWS == k % ROWS)
    ).astype(BF16)
    attn = lax.dot_general(order, mixed, NN, preferred_element_type=F32).astype(BF16)
    lane = iota((width, LANES), 1)
    total = jnp.zeros((width, LANES), F32)
    for t in range(PER):
        for g in range(heads):
            at = g * PER * HD + t * HD
            term = lax.dot_general(w_ref[:, at : at + HD], attn, NN, preferred_element_type=F32)
            total = jnp.where((lane % ROWS == t) & (lane // part == g), term, total)
    place = iota((ROWS, LANES), 1)
    fold = ((place % part) // ROWS == iota((ROWS, LANES), 0)) & (place % ROWS < PER)
    folded = lax.dot_general(
        fold.astype(F32), total, NT, preferred_element_type=F32, precision=lax.Precision.HIGHEST
    )
    out_ref[...] = folded[0:requests, :]


def projected(attn, w_out, requests):
    return pl.pallas_call(
        lambda *refs: project_kernel(requests, *refs),
        in_specs=[vmem()] * 2,
        out_specs=vmem(),
        out_shape=pltpu.VMEM((requests, w_out.shape[1]), F32),
        compiler_params=PARAMS,
        name="project",
    )(near(attn), near(w_out.T))


def attend_kernel(residual_ref, left_ref, right_ref, out_ref, copies_ref):
    attended = (residual_ref[...].astype(F32) + (left_ref[...] + right_ref[...])).astype(BF16)
    out_ref[...] = attended
    for k in range(copies_ref.shape[0]):
        copies_ref[k] = attended


def attend(residual, left, right, copies):
    return pl.pallas_call(
        attend_kernel,
        in_specs=[vmem()] * 3,
        out_specs=[vmem()] * 2,
        out_shape=[
            pltpu.VMEM(residual.shape, BF16),
            pltpu.VMEM((copies, *residual.shape), BF16),
        ],
        compiler_params=PARAMS,
        name="attend",
    )(near(residual), near(left), near(right))


def expert_kernel(x_ref, gain_ref, router_ref, routing_ref, gate_ref, up_ref, down_ref, out_ref):
    requests = x_ref.shape[1]
    model = gain_ref.shape[0]
    held, _, hidden = gate_ref.shape
    experts_all = router_ref.shape[0]
    blocks, _, width = out_ref.shape
    widened = jnp.concatenate([x_ref[k].astype(F32) for k in range(blocks)], axis=1)
    mean_square = jnp.sum(widened * widened, axis=-1, keepdims=True) * (1.0 / model)
    normed = (widened * lax.rsqrt(mean_square + 1e-05) * gain_ref[...].astype(F32).reshape(1, model)).astype(BF16)
    row = iota((requests, experts_all), 0)
    column = iota((requests, experts_all), 1)
    exact = normed.astype(F32)
    logits = jnp.zeros((requests, experts_all), F32)
    for k in range(experts_all):
        logit = jnp.sum(exact * router_ref[k : k + 1, :].astype(F32), axis=-1, keepdims=True)
        logits = jnp.where(column == k, logit, logits)
    picked = []
    for k in range(2):
        chosen = jnp.full((requests, experts_all), routing_ref[k, 0], jnp.int32)
        for r in range(1, requests):
            chosen = jnp.where(row == r, routing_ref[k, r], chosen)
        picked.append(chosen == column)
    ahead = [jnp.sum(jnp.where(p, logits, 0.0), axis=-1, keepdims=True) for p in picked]
    first = jax.nn.sigmoid(ahead[0] - ahead[1])
    combine = jnp.where(picked[0], first, 0.0) + jnp.where(picked[1], 1.0 - first, 0.0)
    core = lax.axis_index(E)
    active = []
    for k in range(held):
        share = jnp.sum(jnp.where(column == core * held + k, combine, 0.0), axis=-1, keepdims=True)
        gate = lax.dot_general(normed, gate_ref[k], NN, preferred_element_type=F32)
        up = lax.dot_general(normed, up_ref[k], NN, preferred_element_type=F32)
        active.append((jax.nn.silu(gate) * up * share).astype(BF16))
    activation = jnp.concatenate(active, axis=-1)
    down = down_ref[...].reshape(held * hidden, model)
    terms = lax.dot_general(activation, down, NN, preferred_element_type=F32)
    for k in range(blocks):
        out_ref[k] = terms[:, k * width : (k + 1) * width]


def experts(gathered, norm_gain, router, routing, w_gate, w_up, w_down, seq_count):
    requests = gathered.shape[1]
    model = norm_gain.shape[0]
    return pl.pallas_call(
        expert_kernel,
        in_specs=[vmem()] * 3 + [pl.BlockSpec(memory_space=pltpu.SMEM)] + [vmem()] * 3,
        out_specs=vmem(),
        out_shape=pltpu.VMEM((seq_count, requests, model // seq_count), F32),
        compiler_params=PARAMS,
        name="experts",
    )(
        near(gathered),
        near(norm_gain),
        near(router.T),
        routing.T,
        near(w_gate),
        near(w_up),
        near(w_down),
    )


def on_device(
    residual,
    queries,
    new_entries,
    kv_cache,
    lengths,
    routing,
    w_out,
    norm_gain,
    router,
    w_gate,
    w_up,
    w_down,
):
    requests = lengths.shape[0]
    seq_count = lax.axis_size(SEQ)
    half_ctx = kv_cache.shape[2] // requests
    mine, limit = packed(queries, new_entries, lengths)
    scores, own, values = partial_scores(mine, swapped(mine), fetched_keys(kv_cache), kv_cache)
    scores, w_gate, w_up, w_down = lax.optimization_barrier((scores, w_gate, w_up, w_down))
    weights = local_weights(to_everyone(scores, X), limit, requests, half_ctx)
    part = weighted_values(to_everyone(weights, X), values, requests)
    attn = merged(own, part, swapped(part), seq_count)
    head_terms = projected(to_everyone(attn, SEQ), w_out, requests)
    attended, copies = attend(residual, head_terms, swapped(head_terms), seq_count)
    gathered = to_everyone(copies, SEQ)
    blocks = experts(gathered, norm_gain, router, routing, w_gate, w_up, w_down, seq_count)
    reduced = to_everyone(blocks, SEQ).sum(axis=0)
    expert_out = (reduced + swapped(reduced)).astype(BF16)
    return (attended, expert_out)


def solution(mesh):
    along_x = mesh.shape["seq"] // KVH
    split = Mesh(
        mesh.devices.reshape(mesh.shape["groups"], KVH, along_x, mesh.shape["expert"]),
        ("groups", Y, X, E),
    )
    return jax.shard_map(
        on_device,
        mesh=split,
        in_specs=(
            P("groups", SEQ),
            P("groups", E),
            P(None, "groups", E),
            P(None, SEQ, ("groups", E)),
            P("groups"),
            P("groups", None),
            P(E, SEQ),
            P(),
            P(),
            P(E, None, SEQ),
            P(E, None, SEQ),
            P(E, SEQ, None),
        ),
        out_specs=(P("groups", SEQ), P("groups", SEQ)),
        check_vma=False,
    )
```

```python
import math

import jax
import jax.numpy as jnp
from jax import lax
from jax.experimental import pallas as pl
from jax.experimental.pallas import tpu as pltpu
from jax.sharding import Mesh
from jax.sharding import PartitionSpec as P

H = 48
KVH = 8
HD = 128
PER = H // KVH
Y = "seq_0"
X = "seq_1"
SEQ = (Y, X)
E = "expert"
LANES = 128
ROWS = 8
FOLD = 4
HEADS = 4
F32 = jnp.float32
BF16 = jnp.bfloat16
LOW = -1e30
LARGEST = 6.0
SCALE = 1.0 / math.sqrt(HD)
PARAMS = pltpu.CompilerParams(vmem_limit_bytes=16 << 20)
NT = (((1,), (1,)), ((), ()))
NN = (((1,), (0,)), ((), ()))


def iota(shape, dim):
    return lax.broadcasted_iota(jnp.int32, shape, dim)


def vmem():
    return pl.BlockSpec(memory_space=pltpu.VMEM)


def exponent_per_unit(depth):
    return 80.0 / (LARGEST * LARGEST * depth * SCALE)


def near(array):
    return pltpu.with_memory_space_constraint(array, pltpu.VMEM)


def far(array):
    return pltpu.with_memory_space_constraint(array, pltpu.HBM)


def swapped(shard):
    return lax.ppermute(shard, E, [(0, 1), (1, 0)])


def to_everyone(copies, axes):
    return lax.all_to_all(copies, axes, split_axis=0, concat_axis=0, tiled=True)


def pack_kernel(q_ref, new_ref, lengths_ref, packed_ref, limit_ref, sizes_ref, sems):
    requests = q_ref.shape[0]
    own_heads = q_ref.shape[1] // (PER * HD)
    local = lax.axis_index(Y) % own_heads
    span = PER * HD
    head = pl.ds(pl.multiple_of(local * HD, LANES), HD)
    copies = [
        pltpu.make_async_copy(lengths_ref, sizes_ref, sems.at[0]),
        pltpu.make_async_copy(
            q_ref.at[:, pl.ds(pl.multiple_of(local * span, LANES), span)], packed_ref.at[:, 0:span], sems.at[1]
        ),
    ]
    for i in range(2):
        copies.append(
            pltpu.make_async_copy(
                new_ref.at[i, :, head], packed_ref.at[:, span + i * HD : span + (i + 1) * HD], sems.at[2 + i]
            )
        )
    for copy in copies:
        copy.start()
    copies[0].wait()
    which = iota((ROWS, LANES), 1) % requests
    limit = jnp.full((ROWS, LANES), sizes_ref[0], jnp.int32)
    for r in range(1, requests):
        limit = jnp.where(which == r, sizes_ref[r], limit)
    limit_ref[...] = limit
    for copy in copies[1:]:
        copy.wait()


def packed(queries, new_entries, lengths):
    requests = queries.shape[0]
    return pl.pallas_call(
        pack_kernel,
        in_specs=[pl.BlockSpec(memory_space=pltpu.HBM)] * 3,
        out_specs=[vmem()] * 2,
        out_shape=[
            pltpu.VMEM((requests, PER * HD + 2 * HD), BF16),
            pltpu.VMEM((ROWS, LANES), jnp.int32),
        ],
        scratch_shapes=[pltpu.SMEM((requests,), jnp.int32), pltpu.SemaphoreType.DMA((4,))],
        compiler_params=PARAMS,
        name="pack",
    )(far(queries), far(new_entries), far(lengths))


def score_kernel(peers, own_heads, mine_ref, other_ref, k_ref, s_ref, own_ref, rows_ref):
    requests = mine_ref.shape[0]
    depth = k_ref.shape[0]
    width = k_ref.shape[1] // peers
    slim = width // FOLD
    x = lax.axis_index(X)
    mine = (lax.axis_index(Y) // own_heads) == lax.axis_index(E)
    q = jnp.where(mine, mine_ref[...].astype(F32), other_ref[...].astype(F32))
    rows_ref[...] = jnp.zeros_like(rows_ref)
    for r in range(requests):
        for t in range(PER):
            rows_ref[r * ROWS + t : r * ROWS + t + 1, :] = q[r : r + 1, t * HD : (t + 1) * HD]
    fresh = [q[:, (PER + i) * HD : (PER + i + 1) * HD].astype(BF16) for i in range(2)]

    rolled = pltpu.roll(rows_ref[0 : requests * ROWS, :], (HD - x * depth) % HD, 1)
    query = rolled[:, 0:depth].astype(BF16)
    which = iota((ROWS, slim), 1) % requests
    for c in range(peers):
        folds = []
        for k in range(FOLD):
            at = c * width + k * slim
            found = lax.dot_general(query, k_ref[:, at : at + slim], NN, preferred_element_type=F32)
            score = found[0:ROWS]
            for r in range(1, requests):
                score = jnp.where(which == r, found[r * ROWS : (r + 1) * ROWS], score)
            folds.append(score[0:PER])
        power = jnp.concatenate(folds, axis=0) * (SCALE * exponent_per_unit(depth))
        s_ref[c] = jnp.exp(power).astype(BF16)

    rows = rows_ref[...].astype(BF16)
    every = lax.dot_general(fresh[0], rows, NT, preferred_element_type=F32)
    own_row = iota(every.shape, 1) // ROWS == iota(every.shape, 0)
    score = jnp.sum(jnp.where(own_row, every, 0.0), axis=0, keepdims=True) * SCALE
    pick = (iota((depth, HD), 1) == iota((depth, HD), 0) + x * depth).astype(BF16)
    values = lax.dot_general(pick, fresh[1], NT, preferred_element_type=F32).astype(BF16)
    spread = (iota((requests, LANES), 1) // ROWS == iota((requests, LANES), 0)).astype(BF16)
    own_ref[0:depth, :] = lax.dot_general(values, spread, NN, preferred_element_type=F32)
    line = iota((ROWS, LANES), 0)
    own_ref[depth : depth + ROWS, :] = jnp.where(line == 0, 1.0, jnp.where(line == 1, score, 0.0))


def key_kernel(kv_ref, k_ref, sem):
    fetch = pltpu.make_async_copy(kv_ref.at[0], k_ref, sem)
    fetch.start()
    fetch.wait()


def fetched_keys(kv_cache):
    return pl.pallas_call(
        key_kernel,
        in_specs=[pl.BlockSpec(memory_space=pltpu.HBM)],
        out_specs=vmem(),
        out_shape=pltpu.VMEM(kv_cache.shape[1:], BF16),
        scratch_shapes=[pltpu.SemaphoreType.DMA],
        compiler_params=PARAMS,
        name="keys",
    )(far(kv_cache))


def partial_scores(mine, other, keys):
    depth = keys.shape[0]
    peers = lax.axis_size(X)
    own_heads = KVH // lax.axis_size(E)
    slim = keys.shape[1] // peers // FOLD
    return pl.pallas_call(
        lambda *refs: score_kernel(peers, own_heads, *refs),
        in_specs=[vmem()] * 3,
        out_specs=[vmem()] * 2,
        out_shape=[pltpu.VMEM((peers, FOLD * PER, slim), BF16), pltpu.VMEM((depth + ROWS, LANES), F32)],
        scratch_shapes=[pltpu.VMEM((LANES, HD), F32)],
        compiler_params=PARAMS,
        name="scores",
    )(near(mine), near(other), near(keys))


def weight_kernel(requests, half_ctx, parts_ref, limit_ref, w_ref):
    peers, tall, slim = parts_ref.shape
    blocks = slim // LANES
    start = lax.axis_index(E) * half_ctx + lax.axis_index(X) * (FOLD * slim // requests)
    limit = jnp.concatenate([limit_ref[...]] * (tall // ROWS), axis=0)
    place = iota((tall, LANES), 1) // requests + start + (iota((tall, LANES), 0) // PER) * (slim // requests)
    scores = []
    high = jnp.full((tall, LANES), LOW, F32)
    for j in range(blocks):
        at = slice(j * LANES, (j + 1) * LANES)
        total = jnp.log(parts_ref[0, :, at].astype(F32))
        for c in range(1, peers):
            total = total + jnp.log(parts_ref[c, :, at].astype(F32))
        alive = place + j * (LANES // requests) < limit
        total = jnp.where(alive, total * (1.0 / exponent_per_unit(HD // peers)), LOW)
        scores.append(total)
        high = jnp.maximum(high, total)
    best = high[0:PER]
    for k in range(1, FOLD):
        best = jnp.maximum(best, high[k * PER : (k + 1) * PER])
    step = requests
    while step < LANES:
        best = jnp.maximum(best, pltpu.roll(best, step, 1))
        step *= 2
    best16 = best.astype(BF16)
    best = best16.astype(F32)
    high = jnp.concatenate([best] * FOLD, axis=0)
    shown = jnp.concatenate([best, jnp.zeros((ROWS - PER, LANES), F32)], axis=0).astype(BF16)
    groups = tall // ROWS
    for j in range(blocks):
        alive = place + j * (LANES // requests) < limit
        weight = jnp.where(alive, jnp.exp(scores[j] - high), 0.0)
        for i in range(groups):
            tile = weight[i * ROWS : (i + 1) * ROWS].astype(BF16)
            for c in range(peers):
                w_ref[c, j * groups + i] = tile
    for c in range(peers):
        w_ref[c, blocks * groups] = shown


def local_weights(parts, limit, requests, half_ctx):
    peers, tall, slim = parts.shape
    tiles = (tall // ROWS) * (slim // LANES) + 1
    return pl.pallas_call(
        lambda *refs: weight_kernel(requests, half_ctx, *refs),
        in_specs=[vmem()] * 2,
        out_specs=vmem(),
        out_shape=pltpu.VMEM((peers, tiles, ROWS, LANES), BF16),
        compiler_params=PARAMS,
        name="weights",
    )(near(parts), near(limit))


def value_kernel(requests, w_ref, v_ref, out_ref):
    peers, tiles = w_ref.shape[:2]
    depth = v_ref.shape[1]
    slim = v_ref.shape[2] // peers // FOLD
    blocks = slim // LANES
    groups = (tiles - 1) // blocks
    used = requests * ROWS
    tops = [w_ref[c, tiles - 1].astype(F32) for c in range(peers)]
    best = tops[0]
    for c in range(1, peers):
        best = jnp.maximum(best, tops[c])
    which = iota((ROWS, slim), 1) % requests
    spare = jnp.zeros((ROWS - PER, slim), F32)
    ones = jnp.ones((depth, slim), BF16)
    acc = jnp.zeros((2 * depth, used), F32)
    for c in range(peers):
        fade = jnp.concatenate([jnp.exp(tops[c] - best)[0:PER]] * FOLD, axis=0)
        weight = jnp.concatenate(
            [
                jnp.concatenate([w_ref[c, j * groups + i].astype(F32) for i in range(groups)], axis=0) * fade
                for j in range(blocks)
            ],
            axis=1,
        )
        for k in range(FOLD):
            part = jnp.concatenate([weight[k * PER : (k + 1) * PER], spare], axis=0)
            masked = jnp.concatenate([jnp.where(which == r, part, 0.0) for r in range(requests)], axis=0)
            at = (c * FOLD + k) * slim
            values = jnp.concatenate([v_ref[1, :, at : at + slim], ones], axis=0)
            acc = acc + lax.dot_general(values, masked.astype(BF16), NT, preferred_element_type=F32)
    lane = iota((ROWS, LANES), 1)
    line = iota((ROWS, LANES), 0)
    mixed = jnp.where((lane // requests == line) & (lane < used), best, 0.0)
    row = jnp.broadcast_to(jnp.sum(mixed, axis=0, keepdims=True), (ROWS, LANES)).astype(BF16)
    a, b = iota((LANES, LANES), 0), iota((LANES, LANES), 1)
    moved = ((a // requests == b % ROWS) & (a % requests == b // ROWS)).astype(BF16)
    top = lax.dot_general(row, moved, NN, preferred_element_type=F32)
    out_ref[...] = jnp.zeros_like(out_ref)
    out_ref[0 : depth + ROWS, 0:used] = acc[0 : depth + ROWS]
    out_ref[depth : depth + ROWS, :] = jnp.where(line == 1, top, out_ref[depth : depth + ROWS, :])


def weighted_values(weights, kv_cache, requests):
    depth = kv_cache.shape[1]
    return pl.pallas_call(
        lambda *refs: value_kernel(requests, *refs),
        in_specs=[vmem()] * 2,
        out_specs=vmem(),
        out_shape=pltpu.VMEM((depth + ROWS, LANES), F32),
        compiler_params=PARAMS,
        name="values",
    )(near(weights), near(kv_cache))


def merge_kernel(own_ref, left_ref, right_ref, out_ref):
    depth = own_ref.shape[0] - ROWS
    parts = (own_ref, left_ref, right_ref)
    highs = [p[depth + 1 : depth + 2, :] for p in parts]
    high = jnp.maximum(jnp.maximum(highs[0], highs[1]), highs[2])
    total = jnp.zeros((1, LANES), F32)
    summed = jnp.zeros((depth, LANES), F32)
    for part, top in zip(parts, highs):
        fade = jnp.exp(top - high)
        total = total + part[depth : depth + 1, :] * fade
        summed = summed + part[0:depth, :] * fade
    attn = summed / total
    held = jnp.zeros((ROWS, LANES), F32)
    for b in range(depth // ROWS):
        held = held + pltpu.roll(attn[b * ROWS : (b + 1) * ROWS], b * (LANES // HEADS), 1)
    held = held.astype(BF16)
    for k in range(out_ref.shape[0]):
        out_ref[k] = held


def merged(own, left, right, copies):
    return pl.pallas_call(
        merge_kernel,
        in_specs=[vmem()] * 3,
        out_specs=vmem(),
        out_shape=pltpu.VMEM((copies, ROWS, LANES), BF16),
        compiler_params=PARAMS,
        name="merge",
    )(near(own), near(left), near(right))


def project_kernel(requests, attn_ref, w_ref, out_ref):
    width = w_ref.shape[0]
    heads = w_ref.shape[1] // (PER * HD)
    along = attn_ref.shape[0] // KVH
    blocks = HD // along // ROWS
    part = LANES // HEADS
    start = lax.axis_index(E) * (heads * along)
    pieces = [
        attn_ref[pl.ds(start + g * along, along)].astype(F32).reshape(along * ROWS, LANES) for g in range(heads)
    ]
    group = iota((along * ROWS, LANES), 1) // part
    stacked = []
    for b in range(blocks):
        mixed = jnp.zeros((along * ROWS, LANES), F32)
        for g in range(heads):
            mixed = jnp.where(group == g, pltpu.roll(pieces[g], ((g - b) * part) % LANES, 1), mixed)
        stacked.append(mixed)
    mixed = jnp.concatenate(stacked, axis=0).astype(BF16)
    d, k = iota((HD, HD), 0), iota((HD, HD), 1)
    order = (
        (d // (blocks * ROWS) == (k // ROWS) % along)
        & ((d // ROWS) % blocks == k // (along * ROWS))
        & (d % ROWS == k % ROWS)
    ).astype(BF16)
    attn = lax.dot_general(order, mixed, NN, preferred_element_type=F32).astype(BF16)
    lane = iota((width, LANES), 1)
    total = jnp.zeros((width, LANES), F32)
    for t in range(PER):
        for g in range(heads):
            at = g * PER * HD + t * HD
            term = lax.dot_general(w_ref[:, at : at + HD], attn, NN, preferred_element_type=F32)
            total = jnp.where((lane % ROWS == t) & (lane // part == g), term, total)
    place = iota((ROWS, LANES), 1)
    fold = ((place % part) // ROWS == iota((ROWS, LANES), 0)) & (place % ROWS < PER)
    folded = lax.dot_general(
        fold.astype(F32), total, NT, preferred_element_type=F32, precision=lax.Precision.HIGHEST
    )
    out_ref[...] = folded[0:requests, :]


def projected(attn, w_out, requests):
    return pl.pallas_call(
        lambda *refs: project_kernel(requests, *refs),
        in_specs=[vmem()] * 2,
        out_specs=vmem(),
        out_shape=pltpu.VMEM((requests, w_out.shape[1]), F32),
        compiler_params=PARAMS,
        name="project",
    )(near(attn), near(w_out.T))


def attend_kernel(residual_ref, left_ref, right_ref, out_ref, copies_ref):
    attended = (residual_ref[...].astype(F32) + (left_ref[...] + right_ref[...])).astype(BF16)
    out_ref[...] = attended
    for k in range(copies_ref.shape[0]):
        copies_ref[k] = attended


def attend(residual, left, right, copies):
    return pl.pallas_call(
        attend_kernel,
        in_specs=[vmem()] * 3,
        out_specs=[vmem()] * 2,
        out_shape=[
            pltpu.VMEM(residual.shape, BF16),
            pltpu.VMEM((copies, *residual.shape), BF16),
        ],
        compiler_params=PARAMS,
        name="attend",
    )(near(residual), near(left), near(right))


def expert_kernel(x_ref, gain_ref, router_ref, routing_ref, gate_ref, up_ref, far_ref, out_ref, down_ref, sem):
    fetch = pltpu.make_async_copy(far_ref, down_ref, sem)
    fetch.start()
    requests = x_ref.shape[1]
    model = gain_ref.shape[0]
    held, _, hidden = gate_ref.shape
    experts_all = router_ref.shape[0]
    blocks, _, width = out_ref.shape
    widened = jnp.concatenate([x_ref[k].astype(F32) for k in range(blocks)], axis=1)
    mean_square = jnp.sum(widened * widened, axis=-1, keepdims=True) * (1.0 / model)
    normed = (widened * lax.rsqrt(mean_square + 1e-05) * gain_ref[...].astype(F32).reshape(1, model)).astype(BF16)
    row = iota((requests, experts_all), 0)
    column = iota((requests, experts_all), 1)
    exact = normed.astype(F32)
    logits = jnp.zeros((requests, experts_all), F32)
    for k in range(experts_all):
        logit = jnp.sum(exact * router_ref[k : k + 1, :].astype(F32), axis=-1, keepdims=True)
        logits = jnp.where(column == k, logit, logits)
    picked = []
    for k in range(2):
        chosen = jnp.full((requests, experts_all), routing_ref[k, 0], jnp.int32)
        for r in range(1, requests):
            chosen = jnp.where(row == r, routing_ref[k, r], chosen)
        picked.append(chosen == column)
    ahead = [jnp.sum(jnp.where(p, logits, 0.0), axis=-1, keepdims=True) for p in picked]
    first = jax.nn.sigmoid(ahead[0] - ahead[1])
    combine = jnp.where(picked[0], first, 0.0) + jnp.where(picked[1], 1.0 - first, 0.0)
    core = lax.axis_index(E)
    active = []
    for k in range(held):
        share = jnp.sum(jnp.where(column == core * held + k, combine, 0.0), axis=-1, keepdims=True)
        gate = lax.dot_general(normed, gate_ref[k], NN, preferred_element_type=F32)
        up = lax.dot_general(normed, up_ref[k], NN, preferred_element_type=F32)
        active.append((jax.nn.silu(gate) * up * share).astype(BF16))
    activation = jnp.concatenate(active, axis=-1)
    fetch.wait()
    down = down_ref[...].reshape(held * hidden, model)
    terms = lax.dot_general(activation, down, NN, preferred_element_type=F32)
    for k in range(blocks):
        out_ref[k] = terms[:, k * width : (k + 1) * width]


def experts(gathered, norm_gain, router, routing, w_gate, w_up, w_down, seq_count):
    requests = gathered.shape[1]
    model = norm_gain.shape[0]
    return pl.pallas_call(
        expert_kernel,
        in_specs=[
            *[vmem()] * 3,
            pl.BlockSpec(memory_space=pltpu.SMEM),
            *[vmem()] * 2,
            pl.BlockSpec(memory_space=pltpu.HBM),
        ],
        out_specs=vmem(),
        scratch_shapes=[pltpu.VMEM(w_down.shape, BF16), pltpu.SemaphoreType.DMA],
        out_shape=pltpu.VMEM((seq_count, requests, model // seq_count), F32),
        compiler_params=PARAMS,
        name="experts",
    )(
        near(gathered),
        near(norm_gain),
        near(router.T),
        routing.T,
        near(w_gate),
        near(w_up),
        far(w_down),
    )


def on_device(
    residual,
    queries,
    new_entries,
    kv_cache,
    lengths,
    routing,
    w_out,
    norm_gain,
    router,
    w_gate,
    w_up,
    w_down,
):
    requests = lengths.shape[0]
    seq_count = lax.axis_size(SEQ)
    half_ctx = kv_cache.shape[2] // requests
    mine, limit = packed(queries, new_entries, lengths)
    scores, own = partial_scores(mine, swapped(mine), fetched_keys(kv_cache))
    weights = local_weights(to_everyone(scores, X), limit, requests, half_ctx)
    part = weighted_values(to_everyone(weights, X), kv_cache, requests)
    attn = merged(own, part, swapped(part), seq_count)
    head_terms = projected(to_everyone(attn, SEQ), w_out, requests)
    attended, copies = attend(residual, head_terms, swapped(head_terms), seq_count)
    gathered = to_everyone(copies, SEQ)
    blocks = experts(gathered, norm_gain, router, routing, w_gate, w_up, w_down, seq_count)
    reduced = to_everyone(blocks, SEQ).sum(axis=0)
    expert_out = (reduced + swapped(reduced)).astype(BF16)
    return (attended, expert_out)


def solution(mesh):
    along_x = mesh.shape["seq"] // KVH
    split = Mesh(
        mesh.devices.reshape(mesh.shape["groups"], KVH, along_x, mesh.shape["expert"]),
        ("groups", Y, X, E),
    )
    return jax.shard_map(
        on_device,
        mesh=split,
        in_specs=(
            P("groups", SEQ),
            P("groups", E),
            P(None, "groups", E),
            P(None, SEQ, ("groups", E)),
            P("groups"),
            P("groups", None),
            P(E, SEQ),
            P(),
            P(),
            P(E, None, SEQ),
            P(E, None, SEQ),
            P(E, SEQ, None),
        ),
        out_specs=(P("groups", SEQ), P("groups", SEQ)),
        check_vma=False,
    )
```

```python
import math

import jax
import jax.numpy as jnp
from jax import lax
from jax.experimental import pallas as pl
from jax.experimental.pallas import tpu as pltpu
from jax.sharding import Mesh
from jax.sharding import PartitionSpec as P

H = 48
KVH = 8
HD = 128
PER = H // KVH
Y = "seq_0"
X = "seq_1"
SEQ = (Y, X)
E = "expert"
LANES = 128
ROWS = 8
FOLD = 4
HEADS = 4
F32 = jnp.float32
BF16 = jnp.bfloat16
LOW = -1e30
LARGEST = 6.0
SCALE = 1.0 / math.sqrt(HD)
PARAMS = pltpu.CompilerParams(vmem_limit_bytes=16 << 20)
NT = (((1,), (1,)), ((), ()))
NN = (((1,), (0,)), ((), ()))


def iota(shape, dim):
    return lax.broadcasted_iota(jnp.int32, shape, dim)


def vmem():
    return pl.BlockSpec(memory_space=pltpu.VMEM)


def exponent_per_unit(depth):
    return 80.0 / (LARGEST * LARGEST * depth * SCALE)


def near(array):
    return pltpu.with_memory_space_constraint(array, pltpu.VMEM)


def far(array):
    return pltpu.with_memory_space_constraint(array, pltpu.HBM)


def swapped(shard):
    return lax.ppermute(shard, E, [(0, 1), (1, 0)])


def to_everyone(copies, axes):
    return lax.all_to_all(copies, axes, split_axis=0, concat_axis=0, tiled=True)


def pack_kernel(q_ref, new_ref, lengths_ref, kv_ref, packed_ref, limit_ref, k_ref, sizes_ref, sems):
    requests = q_ref.shape[0]
    own_heads = q_ref.shape[1] // (PER * HD)
    local = lax.axis_index(Y) % own_heads
    span = PER * HD
    head = pl.ds(pl.multiple_of(local * HD, LANES), HD)
    copies = [
        pltpu.make_async_copy(lengths_ref, sizes_ref, sems.at[0]),
        pltpu.make_async_copy(
            q_ref.at[:, pl.ds(pl.multiple_of(local * span, LANES), span)], packed_ref.at[:, 0:span], sems.at[1]
        ),
    ]
    for i in range(2):
        copies.append(
            pltpu.make_async_copy(
                new_ref.at[i, :, head], packed_ref.at[:, span + i * HD : span + (i + 1) * HD], sems.at[2 + i]
            )
        )
    copies.append(pltpu.make_async_copy(kv_ref.at[0], k_ref, sems.at[4]))
    for copy in copies:
        copy.start()
    copies[0].wait()
    which = iota((ROWS, LANES), 1) % requests
    limit = jnp.full((ROWS, LANES), sizes_ref[0], jnp.int32)
    for r in range(1, requests):
        limit = jnp.where(which == r, sizes_ref[r], limit)
    limit_ref[...] = limit
    for copy in copies[1:]:
        copy.wait()


def packed(queries, new_entries, lengths, kv_cache):
    requests = queries.shape[0]
    return pl.pallas_call(
        pack_kernel,
        in_specs=[pl.BlockSpec(memory_space=pltpu.HBM)] * 4,
        out_specs=[vmem()] * 3,
        out_shape=[
            pltpu.VMEM((requests, PER * HD + 2 * HD), BF16),
            pltpu.VMEM((ROWS, LANES), jnp.int32),
            pltpu.VMEM(kv_cache.shape[1:], BF16),
        ],
        scratch_shapes=[pltpu.SMEM((requests,), jnp.int32), pltpu.SemaphoreType.DMA((5,))],
        compiler_params=PARAMS,
        name="pack",
    )(far(queries), far(new_entries), far(lengths), far(kv_cache))


def score_kernel(peers, own_heads, mine_ref, other_ref, k_ref, s_ref, own_ref, rows_ref):
    requests = mine_ref.shape[0]
    depth = k_ref.shape[0]
    width = k_ref.shape[1] // peers
    slim = width // FOLD
    x = lax.axis_index(X)
    mine = (lax.axis_index(Y) // own_heads) == lax.axis_index(E)
    q = jnp.where(mine, mine_ref[...].astype(F32), other_ref[...].astype(F32))
    rows_ref[...] = jnp.zeros_like(rows_ref)
    for r in range(requests):
        for t in range(PER):
            rows_ref[r * ROWS + t : r * ROWS + t + 1, :] = q[r : r + 1, t * HD : (t + 1) * HD]
    fresh = [q[:, (PER + i) * HD : (PER + i + 1) * HD].astype(BF16) for i in range(2)]

    rolled = pltpu.roll(rows_ref[0 : requests * ROWS, :], (HD - x * depth) % HD, 1)
    query = rolled[:, 0:depth].astype(BF16)
    which = iota((ROWS, slim), 1) % requests
    for c in range(peers):
        folds = []
        for k in range(FOLD):
            at = c * width + k * slim
            found = lax.dot_general(query, k_ref[:, at : at + slim], NN, preferred_element_type=F32)
            score = found[0:ROWS]
            for r in range(1, requests):
                score = jnp.where(which == r, found[r * ROWS : (r + 1) * ROWS], score)
            folds.append(score[0:PER])
        power = jnp.concatenate(folds, axis=0) * (SCALE * exponent_per_unit(depth))
        s_ref[c] = jnp.exp(power).astype(BF16)

    rows = rows_ref[...].astype(BF16)
    every = lax.dot_general(fresh[0], rows, NT, preferred_element_type=F32)
    own_row = iota(every.shape, 1) // ROWS == iota(every.shape, 0)
    score = jnp.sum(jnp.where(own_row, every, 0.0), axis=0, keepdims=True) * SCALE
    pick = (iota((depth, HD), 1) == iota((depth, HD), 0) + x * depth).astype(BF16)
    values = lax.dot_general(pick, fresh[1], NT, preferred_element_type=F32).astype(BF16)
    spread = (iota((requests, LANES), 1) // ROWS == iota((requests, LANES), 0)).astype(BF16)
    own_ref[0:depth, :] = lax.dot_general(values, spread, NN, preferred_element_type=F32)
    line = iota((ROWS, LANES), 0)
    own_ref[depth : depth + ROWS, :] = jnp.where(line == 0, 1.0, jnp.where(line == 1, score, 0.0))


def value_fetch_kernel(kv_ref, v_ref, sem):
    fetch = pltpu.make_async_copy(kv_ref.at[1], v_ref, sem)
    fetch.start()
    fetch.wait()


def fetched_values(kv_cache):
    return pl.pallas_call(
        value_fetch_kernel,
        in_specs=[pl.BlockSpec(memory_space=pltpu.HBM)],
        out_specs=vmem(),
        out_shape=pltpu.VMEM(kv_cache.shape[1:], BF16),
        scratch_shapes=[pltpu.SemaphoreType.DMA],
        compiler_params=PARAMS,
        name="fetch_values",
    )(far(kv_cache))


def partial_scores(mine, other, keys):
    depth = keys.shape[0]
    peers = lax.axis_size(X)
    own_heads = KVH // lax.axis_size(E)
    slim = keys.shape[1] // peers // FOLD
    return pl.pallas_call(
        lambda *refs: score_kernel(peers, own_heads, *refs),
        in_specs=[vmem()] * 3,
        out_specs=[vmem()] * 2,
        out_shape=[pltpu.VMEM((peers, FOLD * PER, slim), BF16), pltpu.VMEM((depth + ROWS, LANES), F32)],
        scratch_shapes=[pltpu.VMEM((LANES, HD), F32)],
        compiler_params=PARAMS,
        name="scores",
    )(near(mine), near(other), near(keys))


def weight_kernel(requests, half_ctx, parts_ref, limit_ref, w_ref):
    peers, tall, slim = parts_ref.shape
    blocks = slim // LANES
    start = lax.axis_index(E) * half_ctx + lax.axis_index(X) * (FOLD * slim // requests)
    limit = jnp.concatenate([limit_ref[...]] * (tall // ROWS), axis=0)
    place = iota((tall, LANES), 1) // requests + start + (iota((tall, LANES), 0) // PER) * (slim // requests)
    scores = []
    high = jnp.full((tall, LANES), LOW, F32)
    for j in range(blocks):
        at = slice(j * LANES, (j + 1) * LANES)
        total = jnp.log(parts_ref[0, :, at].astype(F32))
        for c in range(1, peers):
            total = total + jnp.log(parts_ref[c, :, at].astype(F32))
        alive = place + j * (LANES // requests) < limit
        total = jnp.where(alive, total * (1.0 / exponent_per_unit(HD // peers)), LOW)
        scores.append(total)
        high = jnp.maximum(high, total)
    best = high[0:PER]
    for k in range(1, FOLD):
        best = jnp.maximum(best, high[k * PER : (k + 1) * PER])
    step = requests
    while step < LANES:
        best = jnp.maximum(best, pltpu.roll(best, step, 1))
        step *= 2
    best16 = best.astype(BF16)
    best = best16.astype(F32)
    high = jnp.concatenate([best] * FOLD, axis=0)
    shown = jnp.concatenate([best, jnp.zeros((ROWS - PER, LANES), F32)], axis=0).astype(BF16)
    groups = tall // ROWS
    for j in range(blocks):
        alive = place + j * (LANES // requests) < limit
        weight = jnp.where(alive, jnp.exp(scores[j] - high), 0.0)
        for i in range(groups):
            tile = weight[i * ROWS : (i + 1) * ROWS].astype(BF16)
            for c in range(peers):
                w_ref[c, j * groups + i] = tile
    for c in range(peers):
        w_ref[c, blocks * groups] = shown


def local_weights(parts, limit, requests, half_ctx):
    peers, tall, slim = parts.shape
    tiles = (tall // ROWS) * (slim // LANES) + 1
    return pl.pallas_call(
        lambda *refs: weight_kernel(requests, half_ctx, *refs),
        in_specs=[vmem()] * 2,
        out_specs=vmem(),
        out_shape=pltpu.VMEM((peers, tiles, ROWS, LANES), BF16),
        compiler_params=PARAMS,
        name="weights",
    )(near(parts), near(limit))


def value_kernel(requests, w_ref, v_ref, out_ref):
    peers, tiles = w_ref.shape[:2]
    depth = v_ref.shape[0]
    slim = v_ref.shape[1] // peers // FOLD
    blocks = slim // LANES
    groups = (tiles - 1) // blocks
    used = requests * ROWS
    tops = [w_ref[c, tiles - 1].astype(F32) for c in range(peers)]
    best = tops[0]
    for c in range(1, peers):
        best = jnp.maximum(best, tops[c])
    which = iota((ROWS, slim), 1) % requests
    spare = jnp.zeros((ROWS - PER, slim), F32)
    ones = jnp.ones((depth, slim), BF16)
    acc = jnp.zeros((2 * depth, used), F32)
    for c in range(peers):
        fade = jnp.concatenate([jnp.exp(tops[c] - best)[0:PER]] * FOLD, axis=0)
        weight = jnp.concatenate(
            [
                jnp.concatenate([w_ref[c, j * groups + i].astype(F32) for i in range(groups)], axis=0) * fade
                for j in range(blocks)
            ],
            axis=1,
        )
        for k in range(FOLD):
            part = jnp.concatenate([weight[k * PER : (k + 1) * PER], spare], axis=0)
            masked = jnp.concatenate([jnp.where(which == r, part, 0.0) for r in range(requests)], axis=0)
            at = (c * FOLD + k) * slim
            values = jnp.concatenate([v_ref[:, at : at + slim], ones], axis=0)
            acc = acc + lax.dot_general(values, masked.astype(BF16), NT, preferred_element_type=F32)
    lane = iota((ROWS, LANES), 1)
    line = iota((ROWS, LANES), 0)
    mixed = jnp.where((lane // requests == line) & (lane < used), best, 0.0)
    row = jnp.broadcast_to(jnp.sum(mixed, axis=0, keepdims=True), (ROWS, LANES)).astype(BF16)
    a, b = iota((LANES, LANES), 0), iota((LANES, LANES), 1)
    moved = ((a // requests == b % ROWS) & (a % requests == b // ROWS)).astype(BF16)
    top = lax.dot_general(row, moved, NN, preferred_element_type=F32)
    out_ref[...] = jnp.zeros_like(out_ref)
    out_ref[0 : depth + ROWS, 0:used] = acc[0 : depth + ROWS]
    out_ref[depth : depth + ROWS, :] = jnp.where(line == 1, top, out_ref[depth : depth + ROWS, :])


def weighted_values(weights, values, requests):
    depth = values.shape[0]
    return pl.pallas_call(
        lambda *refs: value_kernel(requests, *refs),
        in_specs=[vmem()] * 2,
        out_specs=vmem(),
        out_shape=pltpu.VMEM((depth + ROWS, LANES), F32),
        compiler_params=PARAMS,
        name="values",
    )(near(weights), near(values))


def merge_kernel(own_ref, left_ref, right_ref, out_ref):
    depth = own_ref.shape[0] - ROWS
    parts = (own_ref, left_ref, right_ref)
    highs = [p[depth + 1 : depth + 2, :] for p in parts]
    high = jnp.maximum(jnp.maximum(highs[0], highs[1]), highs[2])
    total = jnp.zeros((1, LANES), F32)
    summed = jnp.zeros((depth, LANES), F32)
    for part, top in zip(parts, highs):
        fade = jnp.exp(top - high)
        total = total + part[depth : depth + 1, :] * fade
        summed = summed + part[0:depth, :] * fade
    attn = summed / total
    held = jnp.zeros((ROWS, LANES), F32)
    for b in range(depth // ROWS):
        held = held + pltpu.roll(attn[b * ROWS : (b + 1) * ROWS], b * (LANES // HEADS), 1)
    held = held.astype(BF16)
    for k in range(out_ref.shape[0]):
        out_ref[k] = held


def merged(own, left, right, copies):
    return pl.pallas_call(
        merge_kernel,
        in_specs=[vmem()] * 3,
        out_specs=vmem(),
        out_shape=pltpu.VMEM((copies, ROWS, LANES), BF16),
        compiler_params=PARAMS,
        name="merge",
    )(near(own), near(left), near(right))


def project_kernel(requests, attn_ref, w_ref, out_ref):
    width = w_ref.shape[0]
    heads = w_ref.shape[1] // (PER * HD)
    along = attn_ref.shape[0] // KVH
    blocks = HD // along // ROWS
    part = LANES // HEADS
    start = lax.axis_index(E) * (heads * along)
    pieces = [
        attn_ref[pl.ds(start + g * along, along)].astype(F32).reshape(along * ROWS, LANES) for g in range(heads)
    ]
    group = iota((along * ROWS, LANES), 1) // part
    stacked = []
    for b in range(blocks):
        mixed = jnp.zeros((along * ROWS, LANES), F32)
        for g in range(heads):
            mixed = jnp.where(group == g, pltpu.roll(pieces[g], ((g - b) * part) % LANES, 1), mixed)
        stacked.append(mixed)
    mixed = jnp.concatenate(stacked, axis=0).astype(BF16)
    d, k = iota((HD, HD), 0), iota((HD, HD), 1)
    order = (
        (d // (blocks * ROWS) == (k // ROWS) % along)
        & ((d // ROWS) % blocks == k // (along * ROWS))
        & (d % ROWS == k % ROWS)
    ).astype(BF16)
    attn = lax.dot_general(order, mixed, NN, preferred_element_type=F32).astype(BF16)
    lane = iota((width, LANES), 1)
    total = jnp.zeros((width, LANES), F32)
    for t in range(PER):
        for g in range(heads):
            at = g * PER * HD + t * HD
            term = lax.dot_general(w_ref[:, at : at + HD], attn, NN, preferred_element_type=F32)
            total = jnp.where((lane % ROWS == t) & (lane // part == g), term, total)
    place = iota((ROWS, LANES), 1)
    fold = ((place % part) // ROWS == iota((ROWS, LANES), 0)) & (place % ROWS < PER)
    folded = lax.dot_general(
        fold.astype(F32), total, NT, preferred_element_type=F32, precision=lax.Precision.HIGHEST
    )
    out_ref[...] = folded[0:requests, :]


def projected(attn, w_out, requests):
    return pl.pallas_call(
        lambda *refs: project_kernel(requests, *refs),
        in_specs=[vmem()] * 2,
        out_specs=vmem(),
        out_shape=pltpu.VMEM((requests, w_out.shape[1]), F32),
        compiler_params=PARAMS,
        name="project",
    )(near(attn), near(w_out.T))


def attend_kernel(residual_ref, left_ref, right_ref, out_ref, copies_ref):
    attended = (residual_ref[...].astype(F32) + (left_ref[...] + right_ref[...])).astype(BF16)
    out_ref[...] = attended
    for k in range(copies_ref.shape[0]):
        copies_ref[k] = attended


def attend(residual, left, right, copies):
    return pl.pallas_call(
        attend_kernel,
        in_specs=[vmem()] * 3,
        out_specs=[vmem()] * 2,
        out_shape=[
            pltpu.VMEM(residual.shape, BF16),
            pltpu.VMEM((copies, *residual.shape), BF16),
        ],
        compiler_params=PARAMS,
        name="attend",
    )(near(residual), near(left), near(right))


def expert_kernel(x_ref, gain_ref, router_ref, routing_ref, gate_ref, up_ref, down_ref, out_ref):
    requests = x_ref.shape[1]
    model = gain_ref.shape[0]
    held, _, hidden = gate_ref.shape
    experts_all = router_ref.shape[0]
    blocks, _, width = out_ref.shape
    widened = jnp.concatenate([x_ref[k].astype(F32) for k in range(blocks)], axis=1)
    mean_square = jnp.sum(widened * widened, axis=-1, keepdims=True) * (1.0 / model)
    normed = (widened * lax.rsqrt(mean_square + 1e-05) * gain_ref[...].astype(F32).reshape(1, model)).astype(BF16)
    row = iota((requests, experts_all), 0)
    column = iota((requests, experts_all), 1)
    exact = normed.astype(F32)
    logits = jnp.zeros((requests, experts_all), F32)
    for k in range(experts_all):
        logit = jnp.sum(exact * router_ref[k : k + 1, :].astype(F32), axis=-1, keepdims=True)
        logits = jnp.where(column == k, logit, logits)
    picked = []
    for k in range(2):
        chosen = jnp.full((requests, experts_all), routing_ref[k, 0], jnp.int32)
        for r in range(1, requests):
            chosen = jnp.where(row == r, routing_ref[k, r], chosen)
        picked.append(chosen == column)
    ahead = [jnp.sum(jnp.where(p, logits, 0.0), axis=-1, keepdims=True) for p in picked]
    first = jax.nn.sigmoid(ahead[0] - ahead[1])
    combine = jnp.where(picked[0], first, 0.0) + jnp.where(picked[1], 1.0 - first, 0.0)
    core = lax.axis_index(E)
    active = []
    for k in range(held):
        share = jnp.sum(jnp.where(column == core * held + k, combine, 0.0), axis=-1, keepdims=True)
        gate = lax.dot_general(normed, gate_ref[k], NN, preferred_element_type=F32)
        up = lax.dot_general(normed, up_ref[k], NN, preferred_element_type=F32)
        active.append((jax.nn.silu(gate) * up * share).astype(BF16))
    activation = jnp.concatenate(active, axis=-1)
    down = down_ref[...].reshape(held * hidden, model)
    terms = lax.dot_general(activation, down, NN, preferred_element_type=F32)
    for k in range(blocks):
        out_ref[k] = terms[:, k * width : (k + 1) * width]


def experts(gathered, norm_gain, router, routing, w_gate, w_up, w_down, seq_count):
    requests = gathered.shape[1]
    model = norm_gain.shape[0]
    return pl.pallas_call(
        expert_kernel,
        in_specs=[vmem()] * 3 + [pl.BlockSpec(memory_space=pltpu.SMEM)] + [vmem()] * 3,
        out_specs=vmem(),
        out_shape=pltpu.VMEM((seq_count, requests, model // seq_count), F32),
        compiler_params=PARAMS,
        name="experts",
    )(
        near(gathered),
        near(norm_gain),
        near(router.T),
        routing.T,
        near(w_gate),
        near(w_up),
        near(w_down),
    )


def on_device(
    residual,
    queries,
    new_entries,
    kv_cache,
    lengths,
    routing,
    w_out,
    norm_gain,
    router,
    w_gate,
    w_up,
    w_down,
):
    requests = lengths.shape[0]
    seq_count = lax.axis_size(SEQ)
    half_ctx = kv_cache.shape[2] // requests
    mine, limit, keys = packed(queries, new_entries, lengths, kv_cache)
    other = swapped(mine)
    values = fetched_values(kv_cache)
    other, values = lax.optimization_barrier((other, values))
    scores, own = partial_scores(mine, other, keys)
    weights = local_weights(to_everyone(scores, X), limit, requests, half_ctx)
    part = weighted_values(to_everyone(weights, X), values, requests)
    attn = merged(own, part, swapped(part), seq_count)
    head_terms = projected(to_everyone(attn, SEQ), w_out, requests)
    attended, copies = attend(residual, head_terms, swapped(head_terms), seq_count)
    gathered = to_everyone(copies, SEQ)
    blocks = experts(gathered, norm_gain, router, routing, w_gate, w_up, w_down, seq_count)
    reduced = to_everyone(blocks, SEQ).sum(axis=0)
    expert_out = (reduced + swapped(reduced)).astype(BF16)
    return (attended, expert_out)


def solution(mesh):
    along_x = mesh.shape["seq"] // KVH
    split = Mesh(
        mesh.devices.reshape(mesh.shape["groups"], KVH, along_x, mesh.shape["expert"]),
        ("groups", Y, X, E),
    )
    return jax.shard_map(
        on_device,
        mesh=split,
        in_specs=(
            P("groups", SEQ),
            P("groups", E),
            P(None, "groups", E),
            P(None, SEQ, ("groups", E)),
            P("groups"),
            P("groups", None),
            P(E, SEQ),
            P(),
            P(),
            P(E, None, SEQ),
            P(E, None, SEQ),
            P(E, SEQ, None),
        ),
        out_specs=(P("groups", SEQ), P("groups", SEQ)),
        check_vma=False,
    )
```

```python
import math

import jax
import jax.numpy as jnp
from jax import lax
from jax.experimental import pallas as pl
from jax.experimental.pallas import tpu as pltpu
from jax.sharding import Mesh
from jax.sharding import PartitionSpec as P

H = 48
KVH = 8
HD = 128
PER = H // KVH
Y = "seq_0"
X = "seq_1"
SEQ = (Y, X)
E = "expert"
LANES = 128
ROWS = 8
FOLD = 4
HEADS = 4
F32 = jnp.float32
BF16 = jnp.bfloat16
LOW = -1e30
LARGEST = 6.0
SCALE = 1.0 / math.sqrt(HD)
AFTER_TRANSFER = pl.CostEstimate(flops=20_000_000_000, transcendentals=0, bytes_accessed=1 << 24)
PARAMS = pltpu.CompilerParams(vmem_limit_bytes=16 << 20)
NT = (((1,), (1,)), ((), ()))
NN = (((1,), (0,)), ((), ()))


def iota(shape, dim):
    return lax.broadcasted_iota(jnp.int32, shape, dim)


def vmem():
    return pl.BlockSpec(memory_space=pltpu.VMEM)


def exponent_per_unit(depth):
    return 80.0 / (LARGEST * LARGEST * depth * SCALE)


def near(array):
    return pltpu.with_memory_space_constraint(array, pltpu.VMEM)


def far(array):
    return pltpu.with_memory_space_constraint(array, pltpu.HBM)


def swapped(shard):
    return lax.ppermute(shard, E, [(0, 1), (1, 0)])


def to_everyone(copies, axes):
    return lax.all_to_all(copies, axes, split_axis=0, concat_axis=0, tiled=True)


def pack_kernel(q_ref, new_ref, lengths_ref, kv_ref, packed_ref, limit_ref, k_ref, sizes_ref, sems):
    requests = q_ref.shape[0]
    own_heads = q_ref.shape[1] // (PER * HD)
    local = lax.axis_index(Y) % own_heads
    span = PER * HD
    head = pl.ds(pl.multiple_of(local * HD, LANES), HD)
    copies = [
        pltpu.make_async_copy(lengths_ref, sizes_ref, sems.at[0]),
        pltpu.make_async_copy(
            q_ref.at[:, pl.ds(pl.multiple_of(local * span, LANES), span)], packed_ref.at[:, 0:span], sems.at[1]
        ),
    ]
    for i in range(2):
        copies.append(
            pltpu.make_async_copy(
                new_ref.at[i, :, head], packed_ref.at[:, span + i * HD : span + (i + 1) * HD], sems.at[2 + i]
            )
        )
    copies.append(pltpu.make_async_copy(kv_ref.at[0], k_ref, sems.at[4]))
    for copy in copies:
        copy.start()
    copies[0].wait()
    which = iota((ROWS, LANES), 1) % requests
    limit = jnp.full((ROWS, LANES), sizes_ref[0], jnp.int32)
    for r in range(1, requests):
        limit = jnp.where(which == r, sizes_ref[r], limit)
    limit_ref[...] = limit
    for copy in copies[1:]:
        copy.wait()


def packed(queries, new_entries, lengths, kv_cache):
    requests = queries.shape[0]
    return pl.pallas_call(
        pack_kernel,
        in_specs=[pl.BlockSpec(memory_space=pltpu.HBM)] * 4,
        out_specs=[vmem()] * 3,
        out_shape=[
            pltpu.VMEM((requests, PER * HD + 2 * HD), BF16),
            pltpu.VMEM((ROWS, LANES), jnp.int32),
            pltpu.VMEM(kv_cache.shape[1:], BF16),
        ],
        scratch_shapes=[pltpu.SMEM((requests,), jnp.int32), pltpu.SemaphoreType.DMA((5,))],
        compiler_params=PARAMS,
        name="pack",
    )(far(queries), far(new_entries), far(lengths), far(kv_cache))


def score_kernel(peers, own_heads, mine_ref, other_ref, k_ref, s_ref, own_ref, rows_ref):
    requests = mine_ref.shape[0]
    depth = k_ref.shape[0]
    width = k_ref.shape[1] // peers
    slim = width // FOLD
    x = lax.axis_index(X)
    mine = (lax.axis_index(Y) // own_heads) == lax.axis_index(E)
    q = jnp.where(mine, mine_ref[...].astype(F32), other_ref[...].astype(F32))
    rows_ref[...] = jnp.zeros_like(rows_ref)
    for r in range(requests):
        for t in range(PER):
            rows_ref[r * ROWS + t : r * ROWS + t + 1, :] = q[r : r + 1, t * HD : (t + 1) * HD]
    fresh = [q[:, (PER + i) * HD : (PER + i + 1) * HD].astype(BF16) for i in range(2)]

    rolled = pltpu.roll(rows_ref[0 : requests * ROWS, :], (HD - x * depth) % HD, 1)
    query = rolled[:, 0:depth].astype(BF16)
    which = iota((ROWS, slim), 1) % requests
    for c in range(peers):
        folds = []
        for k in range(FOLD):
            at = c * width + k * slim
            found = lax.dot_general(query, k_ref[:, at : at + slim], NN, preferred_element_type=F32)
            score = found[0:ROWS]
            for r in range(1, requests):
                score = jnp.where(which == r, found[r * ROWS : (r + 1) * ROWS], score)
            folds.append(score[0:PER])
        power = jnp.concatenate(folds, axis=0) * (SCALE * exponent_per_unit(depth))
        s_ref[c] = jnp.exp(power).astype(BF16)

    rows = rows_ref[...].astype(BF16)
    every = lax.dot_general(fresh[0], rows, NT, preferred_element_type=F32)
    own_row = iota(every.shape, 1) // ROWS == iota(every.shape, 0)
    score = jnp.sum(jnp.where(own_row, every, 0.0), axis=0, keepdims=True) * SCALE
    pick = (iota((depth, HD), 1) == iota((depth, HD), 0) + x * depth).astype(BF16)
    values = lax.dot_general(pick, fresh[1], NT, preferred_element_type=F32).astype(BF16)
    spread = (iota((requests, LANES), 1) // ROWS == iota((requests, LANES), 0)).astype(BF16)
    own_ref[0:depth, :] = lax.dot_general(values, spread, NN, preferred_element_type=F32)
    line = iota((ROWS, LANES), 0)
    own_ref[depth : depth + ROWS, :] = jnp.where(line == 0, 1.0, jnp.where(line == 1, score, 0.0))


def value_fetch_kernel(kv_ref, v_ref, sem):
    fetch = pltpu.make_async_copy(kv_ref.at[1], v_ref, sem)
    fetch.start()
    fetch.wait()


def fetched_values(kv_cache):
    return pl.pallas_call(
        value_fetch_kernel,
        in_specs=[pl.BlockSpec(memory_space=pltpu.HBM)],
        out_specs=vmem(),
        out_shape=pltpu.VMEM(kv_cache.shape[1:], BF16),
        scratch_shapes=[pltpu.SemaphoreType.DMA],
        compiler_params=PARAMS,
        name="fetch_values",
    )(far(kv_cache))


def partial_scores(mine, other, keys):
    depth = keys.shape[0]
    peers = lax.axis_size(X)
    own_heads = KVH // lax.axis_size(E)
    slim = keys.shape[1] // peers // FOLD
    return pl.pallas_call(
        lambda *refs: score_kernel(peers, own_heads, *refs),
        in_specs=[vmem()] * 3,
        out_specs=[vmem()] * 2,
        out_shape=[pltpu.VMEM((peers, FOLD * PER, slim), BF16), pltpu.VMEM((depth + ROWS, LANES), F32)],
        scratch_shapes=[pltpu.VMEM((LANES, HD), F32)],
        compiler_params=PARAMS,
        name="scores",
    )(near(mine), near(other), near(keys))


def weight_kernel(requests, half_ctx, parts_ref, limit_ref, w_ref):
    peers, tall, slim = parts_ref.shape
    blocks = slim // LANES
    start = lax.axis_index(E) * half_ctx + lax.axis_index(X) * (FOLD * slim // requests)
    limit = jnp.concatenate([limit_ref[...]] * (tall // ROWS), axis=0)
    place = iota((tall, LANES), 1) // requests + start + (iota((tall, LANES), 0) // PER) * (slim // requests)
    scores = []
    high = jnp.full((tall, LANES), LOW, F32)
    for j in range(blocks):
        at = slice(j * LANES, (j + 1) * LANES)
        total = jnp.log(parts_ref[0, :, at].astype(F32))
        for c in range(1, peers):
            total = total + jnp.log(parts_ref[c, :, at].astype(F32))
        alive = place + j * (LANES // requests) < limit
        total = jnp.where(alive, total * (1.0 / exponent_per_unit(HD // peers)), LOW)
        scores.append(total)
        high = jnp.maximum(high, total)
    best = high[0:PER]
    for k in range(1, FOLD):
        best = jnp.maximum(best, high[k * PER : (k + 1) * PER])
    step = requests
    while step < LANES:
        best = jnp.maximum(best, pltpu.roll(best, step, 1))
        step *= 2
    best16 = best.astype(BF16)
    best = best16.astype(F32)
    high = jnp.concatenate([best] * FOLD, axis=0)
    shown = jnp.concatenate([best, jnp.zeros((ROWS - PER, LANES), F32)], axis=0).astype(BF16)
    groups = tall // ROWS
    for j in range(blocks):
        alive = place + j * (LANES // requests) < limit
        weight = jnp.where(alive, jnp.exp(scores[j] - high), 0.0)
        for i in range(groups):
            tile = weight[i * ROWS : (i + 1) * ROWS].astype(BF16)
            for c in range(peers):
                w_ref[c, j * groups + i] = tile
    for c in range(peers):
        w_ref[c, blocks * groups] = shown


def local_weights(parts, limit, requests, half_ctx):
    peers, tall, slim = parts.shape
    tiles = (tall // ROWS) * (slim // LANES) + 1
    return pl.pallas_call(
        lambda *refs: weight_kernel(requests, half_ctx, *refs),
        in_specs=[vmem()] * 2,
        out_specs=vmem(),
        out_shape=pltpu.VMEM((peers, tiles, ROWS, LANES), BF16),
        compiler_params=PARAMS,
        cost_estimate=AFTER_TRANSFER,
        name="weights",
    )(near(parts), near(limit))


def value_kernel(requests, w_ref, v_ref, out_ref):
    peers, tiles = w_ref.shape[:2]
    depth = v_ref.shape[0]
    slim = v_ref.shape[1] // peers // FOLD
    blocks = slim // LANES
    groups = (tiles - 1) // blocks
    used = requests * ROWS
    tops = [w_ref[c, tiles - 1].astype(F32) for c in range(peers)]
    best = tops[0]
    for c in range(1, peers):
        best = jnp.maximum(best, tops[c])
    which = iota((ROWS, slim), 1) % requests
    spare = jnp.zeros((ROWS - PER, slim), F32)
    ones = jnp.ones((depth, slim), BF16)
    acc = jnp.zeros((2 * depth, used), F32)
    for c in range(peers):
        fade = jnp.concatenate([jnp.exp(tops[c] - best)[0:PER]] * FOLD, axis=0)
        weight = jnp.concatenate(
            [
                jnp.concatenate([w_ref[c, j * groups + i].astype(F32) for i in range(groups)], axis=0) * fade
                for j in range(blocks)
            ],
            axis=1,
        )
        for k in range(FOLD):
            part = jnp.concatenate([weight[k * PER : (k + 1) * PER], spare], axis=0)
            masked = jnp.concatenate([jnp.where(which == r, part, 0.0) for r in range(requests)], axis=0)
            at = (c * FOLD + k) * slim
            values = jnp.concatenate([v_ref[:, at : at + slim], ones], axis=0)
            acc = acc + lax.dot_general(values, masked.astype(BF16), NT, preferred_element_type=F32)
    lane = iota((ROWS, LANES), 1)
    line = iota((ROWS, LANES), 0)
    mixed = jnp.where((lane // requests == line) & (lane < used), best, 0.0)
    row = jnp.broadcast_to(jnp.sum(mixed, axis=0, keepdims=True), (ROWS, LANES)).astype(BF16)
    a, b = iota((LANES, LANES), 0), iota((LANES, LANES), 1)
    moved = ((a // requests == b % ROWS) & (a % requests == b // ROWS)).astype(BF16)
    top = lax.dot_general(row, moved, NN, preferred_element_type=F32)
    out_ref[...] = jnp.zeros_like(out_ref)
    out_ref[0 : depth + ROWS, 0:used] = acc[0 : depth + ROWS]
    out_ref[depth : depth + ROWS, :] = jnp.where(line == 1, top, out_ref[depth : depth + ROWS, :])


def weighted_values(weights, values, requests):
    depth = values.shape[0]
    return pl.pallas_call(
        lambda *refs: value_kernel(requests, *refs),
        in_specs=[vmem()] * 2,
        out_specs=vmem(),
        out_shape=pltpu.VMEM((depth + ROWS, LANES), F32),
        compiler_params=PARAMS,
        cost_estimate=AFTER_TRANSFER,
        name="values",
    )(near(weights), near(values))


def merge_kernel(own_ref, left_ref, right_ref, out_ref):
    depth = own_ref.shape[0] - ROWS
    parts = (own_ref, left_ref, right_ref)
    highs = [p[depth + 1 : depth + 2, :] for p in parts]
    high = jnp.maximum(jnp.maximum(highs[0], highs[1]), highs[2])
    total = jnp.zeros((1, LANES), F32)
    summed = jnp.zeros((depth, LANES), F32)
    for part, top in zip(parts, highs):
        fade = jnp.exp(top - high)
        total = total + part[depth : depth + 1, :] * fade
        summed = summed + part[0:depth, :] * fade
    attn = summed / total
    held = jnp.zeros((ROWS, LANES), F32)
    for b in range(depth // ROWS):
        held = held + pltpu.roll(attn[b * ROWS : (b + 1) * ROWS], b * (LANES // HEADS), 1)
    held = held.astype(BF16)
    for k in range(out_ref.shape[0]):
        out_ref[k] = held


def merged(own, left, right, copies):
    return pl.pallas_call(
        merge_kernel,
        in_specs=[vmem()] * 3,
        out_specs=vmem(),
        out_shape=pltpu.VMEM((copies, ROWS, LANES), BF16),
        compiler_params=PARAMS,
        cost_estimate=AFTER_TRANSFER,
        name="merge",
    )(near(own), near(left), near(right))


def project_kernel(requests, attn_ref, w_ref, out_ref):
    width = w_ref.shape[0]
    heads = w_ref.shape[1] // (PER * HD)
    along = attn_ref.shape[0] // KVH
    blocks = HD // along // ROWS
    part = LANES // HEADS
    start = lax.axis_index(E) * (heads * along)
    pieces = [
        attn_ref[pl.ds(start + g * along, along)].astype(F32).reshape(along * ROWS, LANES) for g in range(heads)
    ]
    group = iota((along * ROWS, LANES), 1) // part
    stacked = []
    for b in range(blocks):
        mixed = jnp.zeros((along * ROWS, LANES), F32)
        for g in range(heads):
            mixed = jnp.where(group == g, pltpu.roll(pieces[g], ((g - b) * part) % LANES, 1), mixed)
        stacked.append(mixed)
    mixed = jnp.concatenate(stacked, axis=0).astype(BF16)
    d, k = iota((HD, HD), 0), iota((HD, HD), 1)
    order = (
        (d // (blocks * ROWS) == (k // ROWS) % along)
        & ((d // ROWS) % blocks == k // (along * ROWS))
        & (d % ROWS == k % ROWS)
    ).astype(BF16)
    attn = lax.dot_general(order, mixed, NN, preferred_element_type=F32).astype(BF16)
    lane = iota((width, LANES), 1)
    total = jnp.zeros((width, LANES), F32)
    for t in range(PER):
        for g in range(heads):
            at = g * PER * HD + t * HD
            term = lax.dot_general(w_ref[:, at : at + HD], attn, NN, preferred_element_type=F32)
            total = jnp.where((lane % ROWS == t) & (lane // part == g), term, total)
    place = iota((ROWS, LANES), 1)
    fold = ((place % part) // ROWS == iota((ROWS, LANES), 0)) & (place % ROWS < PER)
    folded = lax.dot_general(
        fold.astype(F32), total, NT, preferred_element_type=F32, precision=lax.Precision.HIGHEST
    )
    out_ref[...] = folded[0:requests, :]


def projected(attn, w_out, requests):
    return pl.pallas_call(
        lambda *refs: project_kernel(requests, *refs),
        in_specs=[vmem()] * 2,
        out_specs=vmem(),
        out_shape=pltpu.VMEM((requests, w_out.shape[1]), F32),
        compiler_params=PARAMS,
        cost_estimate=AFTER_TRANSFER,
        name="project",
    )(near(attn), near(w_out.T))


def attend_kernel(residual_ref, left_ref, right_ref, out_ref, copies_ref):
    attended = (residual_ref[...].astype(F32) + (left_ref[...] + right_ref[...])).astype(BF16)
    out_ref[...] = attended
    for k in range(copies_ref.shape[0]):
        copies_ref[k] = attended


def attend(residual, left, right, copies):
    return pl.pallas_call(
        attend_kernel,
        in_specs=[vmem()] * 3,
        out_specs=[vmem()] * 2,
        out_shape=[
            pltpu.VMEM(residual.shape, BF16),
            pltpu.VMEM((copies, *residual.shape), BF16),
        ],
        compiler_params=PARAMS,
        cost_estimate=AFTER_TRANSFER,
        name="attend",
    )(near(residual), near(left), near(right))


def expert_kernel(x_ref, gain_ref, router_ref, routing_ref, gate_ref, up_ref, down_ref, out_ref):
    requests = x_ref.shape[1]
    model = gain_ref.shape[0]
    held, _, hidden = gate_ref.shape
    experts_all = router_ref.shape[0]
    blocks, _, width = out_ref.shape
    widened = jnp.concatenate([x_ref[k].astype(F32) for k in range(blocks)], axis=1)
    mean_square = jnp.sum(widened * widened, axis=-1, keepdims=True) * (1.0 / model)
    normed = (widened * lax.rsqrt(mean_square + 1e-05) * gain_ref[...].astype(F32).reshape(1, model)).astype(BF16)
    row = iota((requests, experts_all), 0)
    column = iota((requests, experts_all), 1)
    exact = normed.astype(F32)
    logits = jnp.zeros((requests, experts_all), F32)
    for k in range(experts_all):
        logit = jnp.sum(exact * router_ref[k : k + 1, :].astype(F32), axis=-1, keepdims=True)
        logits = jnp.where(column == k, logit, logits)
    picked = []
    for k in range(2):
        chosen = jnp.full((requests, experts_all), routing_ref[k, 0], jnp.int32)
        for r in range(1, requests):
            chosen = jnp.where(row == r, routing_ref[k, r], chosen)
        picked.append(chosen == column)
    ahead = [jnp.sum(jnp.where(p, logits, 0.0), axis=-1, keepdims=True) for p in picked]
    first = jax.nn.sigmoid(ahead[0] - ahead[1])
    combine = jnp.where(picked[0], first, 0.0) + jnp.where(picked[1], 1.0 - first, 0.0)
    core = lax.axis_index(E)
    active = []
    for k in range(held):
        share = jnp.sum(jnp.where(column == core * held + k, combine, 0.0), axis=-1, keepdims=True)
        gate = lax.dot_general(normed, gate_ref[k], NN, preferred_element_type=F32)
        up = lax.dot_general(normed, up_ref[k], NN, preferred_element_type=F32)
        active.append((jax.nn.silu(gate) * up * share).astype(BF16))
    activation = jnp.concatenate(active, axis=-1)
    down = down_ref[...].reshape(held * hidden, model)
    terms = lax.dot_general(activation, down, NN, preferred_element_type=F32)
    for k in range(blocks):
        out_ref[k] = terms[:, k * width : (k + 1) * width]


def experts(gathered, norm_gain, router, routing, w_gate, w_up, w_down, seq_count):
    requests = gathered.shape[1]
    model = norm_gain.shape[0]
    return pl.pallas_call(
        expert_kernel,
        in_specs=[vmem()] * 3 + [pl.BlockSpec(memory_space=pltpu.SMEM)] + [vmem()] * 3,
        out_specs=vmem(),
        out_shape=pltpu.VMEM((seq_count, requests, model // seq_count), F32),
        compiler_params=PARAMS,
        name="experts",
    )(
        near(gathered),
        near(norm_gain),
        near(router.T),
        routing.T,
        near(w_gate),
        near(w_up),
        near(w_down),
    )


def on_device(
    residual,
    queries,
    new_entries,
    kv_cache,
    lengths,
    routing,
    w_out,
    norm_gain,
    router,
    w_gate,
    w_up,
    w_down,
):
    requests = lengths.shape[0]
    seq_count = lax.axis_size(SEQ)
    half_ctx = kv_cache.shape[2] // requests
    mine, limit, keys = packed(queries, new_entries, lengths, kv_cache)
    other = swapped(mine)
    values = fetched_values(kv_cache)
    other, values = lax.optimization_barrier((other, values))
    scores, own = partial_scores(mine, other, keys)
    weights = local_weights(to_everyone(scores, X), limit, requests, half_ctx)
    part = weighted_values(to_everyone(weights, X), values, requests)
    attn = merged(own, part, swapped(part), seq_count)
    head_terms = projected(to_everyone(attn, SEQ), w_out, requests)
    attended, copies = attend(residual, head_terms, swapped(head_terms), seq_count)
    gathered = to_everyone(copies, SEQ)
    blocks = experts(gathered, norm_gain, router, routing, w_gate, w_up, w_down, seq_count)
    reduced = to_everyone(blocks, SEQ).sum(axis=0)
    expert_out = (reduced + swapped(reduced)).astype(BF16)
    return (attended, expert_out)


def solution(mesh):
    along_x = mesh.shape["seq"] // KVH
    split = Mesh(
        mesh.devices.reshape(mesh.shape["groups"], KVH, along_x, mesh.shape["expert"]),
        ("groups", Y, X, E),
    )
    return jax.shard_map(
        on_device,
        mesh=split,
        in_specs=(
            P("groups", SEQ),
            P("groups", E),
            P(None, "groups", E),
            P(None, SEQ, ("groups", E)),
            P("groups"),
            P("groups", None),
            P(E, SEQ),
            P(),
            P(),
            P(E, None, SEQ),
            P(E, None, SEQ),
            P(E, SEQ, None),
        ),
        out_specs=(P("groups", SEQ), P("groups", SEQ)),
        check_vma=False,
    )
```

```python
import math

import jax
import jax.numpy as jnp
from jax import lax
from jax.experimental import pallas as pl
from jax.experimental.pallas import tpu as pltpu
from jax.sharding import Mesh
from jax.sharding import PartitionSpec as P

H = 48
KVH = 8
HD = 128
PER = H // KVH
Y = "seq_0"
X = "seq_1"
SEQ = (Y, X)
E = "expert"
LANES = 128
ROWS = 8
FOLD = 4
HEADS = 4
F32 = jnp.float32
BF16 = jnp.bfloat16
LOW = -1e30
LARGEST = 6.0
SCALE = 1.0 / math.sqrt(HD)
AFTER_TRANSFER = pl.CostEstimate(flops=20_000_000_000, transcendentals=0, bytes_accessed=1 << 24)
PARAMS = pltpu.CompilerParams(vmem_limit_bytes=16 << 20)
NT = (((1,), (1,)), ((), ()))
NN = (((1,), (0,)), ((), ()))


def iota(shape, dim):
    return lax.broadcasted_iota(jnp.int32, shape, dim)


def vmem():
    return pl.BlockSpec(memory_space=pltpu.VMEM)


def exponent_per_unit(depth):
    return 80.0 / (LARGEST * LARGEST * depth * SCALE)


def near(array):
    return pltpu.with_memory_space_constraint(array, pltpu.VMEM)


def far(array):
    return pltpu.with_memory_space_constraint(array, pltpu.HBM)


def swapped(shard):
    return lax.ppermute(shard, E, [(0, 1), (1, 0)])


def to_everyone(copies, axes):
    return lax.all_to_all(copies, axes, split_axis=0, concat_axis=0, tiled=True)


def pack_kernel(q_ref, new_ref, lengths_ref, packed_ref, limit_ref, sizes_ref, sems):
    requests = q_ref.shape[0]
    own_heads = q_ref.shape[1] // (PER * HD)
    local = lax.axis_index(Y) % own_heads
    span = PER * HD
    head = pl.ds(pl.multiple_of(local * HD, LANES), HD)
    copies = [
        pltpu.make_async_copy(lengths_ref, sizes_ref, sems.at[0]),
        pltpu.make_async_copy(
            q_ref.at[:, pl.ds(pl.multiple_of(local * span, LANES), span)], packed_ref.at[:, 0:span], sems.at[1]
        ),
    ]
    for i in range(2):
        copies.append(
            pltpu.make_async_copy(
                new_ref.at[i, :, head], packed_ref.at[:, span + i * HD : span + (i + 1) * HD], sems.at[2 + i]
            )
        )
    for copy in copies:
        copy.start()
    copies[0].wait()
    which = iota((ROWS, LANES), 1) % requests
    limit = jnp.full((ROWS, LANES), sizes_ref[0], jnp.int32)
    for r in range(1, requests):
        limit = jnp.where(which == r, sizes_ref[r], limit)
    limit_ref[...] = limit
    for copy in copies[1:]:
        copy.wait()


def packed(queries, new_entries, lengths):
    requests = queries.shape[0]
    return pl.pallas_call(
        pack_kernel,
        in_specs=[pl.BlockSpec(memory_space=pltpu.HBM)] * 3,
        out_specs=[vmem()] * 2,
        out_shape=[
            pltpu.VMEM((requests, PER * HD + 2 * HD), BF16),
            pltpu.VMEM((ROWS, LANES), jnp.int32),
        ],
        scratch_shapes=[pltpu.SMEM((requests,), jnp.int32), pltpu.SemaphoreType.DMA((4,))],
        compiler_params=PARAMS,
        name="pack",
    )(far(queries), far(new_entries), far(lengths))


def score_kernel(peers, own_heads, mine_ref, other_ref, k_ref, s_ref, own_ref, rows_ref):
    requests = mine_ref.shape[0]
    depth = k_ref.shape[0]
    width = k_ref.shape[1] // peers
    slim = width // FOLD
    x = lax.axis_index(X)
    mine = (lax.axis_index(Y) // own_heads) == lax.axis_index(E)
    q = jnp.where(mine, mine_ref[...].astype(F32), other_ref[...].astype(F32))
    rows_ref[...] = jnp.zeros_like(rows_ref)
    for r in range(requests):
        for t in range(PER):
            rows_ref[r * ROWS + t : r * ROWS + t + 1, :] = q[r : r + 1, t * HD : (t + 1) * HD]
    fresh = [q[:, (PER + i) * HD : (PER + i + 1) * HD].astype(BF16) for i in range(2)]

    rolled = pltpu.roll(rows_ref[0 : requests * ROWS, :], (HD - x * depth) % HD, 1)
    query = rolled[:, 0:depth].astype(BF16)
    which = iota((ROWS, slim), 1) % requests
    for c in range(peers):
        folds = []
        for k in range(FOLD):
            at = c * width + k * slim
            found = lax.dot_general(query, k_ref[:, at : at + slim], NN, preferred_element_type=F32)
            score = found[0:ROWS]
            for r in range(1, requests):
                score = jnp.where(which == r, found[r * ROWS : (r + 1) * ROWS], score)
            folds.append(score[0:PER])
        power = jnp.concatenate(folds, axis=0) * (SCALE * exponent_per_unit(depth))
        s_ref[c] = jnp.exp(power).astype(BF16)

    rows = rows_ref[...].astype(BF16)
    every = lax.dot_general(fresh[0], rows, NT, preferred_element_type=F32)
    own_row = iota(every.shape, 1) // ROWS == iota(every.shape, 0)
    score = jnp.sum(jnp.where(own_row, every, 0.0), axis=0, keepdims=True) * SCALE
    pick = (iota((depth, HD), 1) == iota((depth, HD), 0) + x * depth).astype(BF16)
    values = lax.dot_general(pick, fresh[1], NT, preferred_element_type=F32).astype(BF16)
    spread = (iota((requests, LANES), 1) // ROWS == iota((requests, LANES), 0)).astype(BF16)
    own_ref[0:depth, :] = lax.dot_general(values, spread, NN, preferred_element_type=F32)
    line = iota((ROWS, LANES), 0)
    own_ref[depth : depth + ROWS, :] = jnp.where(line == 0, 1.0, jnp.where(line == 1, score, 0.0))


def key_kernel(kv_ref, k_ref, sem):
    fetch = pltpu.make_async_copy(kv_ref.at[0], k_ref, sem)
    fetch.start()
    fetch.wait()


def fetched_keys(kv_cache):
    return pl.pallas_call(
        key_kernel,
        in_specs=[pl.BlockSpec(memory_space=pltpu.HBM)],
        out_specs=vmem(),
        out_shape=pltpu.VMEM(kv_cache.shape[1:], BF16),
        scratch_shapes=[pltpu.SemaphoreType.DMA],
        compiler_params=PARAMS,
        name="keys",
    )(far(kv_cache))


def partial_scores(mine, other, keys):
    depth = keys.shape[0]
    peers = lax.axis_size(X)
    own_heads = KVH // lax.axis_size(E)
    slim = keys.shape[1] // peers // FOLD
    return pl.pallas_call(
        lambda *refs: score_kernel(peers, own_heads, *refs),
        in_specs=[vmem()] * 3,
        out_specs=[vmem()] * 2,
        out_shape=[pltpu.VMEM((peers, FOLD * PER, slim), BF16), pltpu.VMEM((depth + ROWS, LANES), F32)],
        scratch_shapes=[pltpu.VMEM((LANES, HD), F32)],
        compiler_params=PARAMS,
        name="scores",
    )(near(mine), near(other), near(keys))


def weight_kernel(requests, half_ctx, parts_ref, limit_ref, w_ref):
    peers, tall, slim = parts_ref.shape
    blocks = slim // LANES
    start = lax.axis_index(E) * half_ctx + lax.axis_index(X) * (FOLD * slim // requests)
    limit = jnp.concatenate([limit_ref[...]] * (tall // ROWS), axis=0)
    place = iota((tall, LANES), 1) // requests + start + (iota((tall, LANES), 0) // PER) * (slim // requests)
    scores = []
    high = jnp.full((tall, LANES), LOW, F32)
    for j in range(blocks):
        at = slice(j * LANES, (j + 1) * LANES)
        total = jnp.log(parts_ref[0, :, at].astype(F32))
        for c in range(1, peers):
            total = total + jnp.log(parts_ref[c, :, at].astype(F32))
        alive = place + j * (LANES // requests) < limit
        total = jnp.where(alive, total * (1.0 / exponent_per_unit(HD // peers)), LOW)
        scores.append(total)
        high = jnp.maximum(high, total)
    best = high[0:PER]
    for k in range(1, FOLD):
        best = jnp.maximum(best, high[k * PER : (k + 1) * PER])
    step = requests
    while step < LANES:
        best = jnp.maximum(best, pltpu.roll(best, step, 1))
        step *= 2
    best16 = best.astype(BF16)
    best = best16.astype(F32)
    high = jnp.concatenate([best] * FOLD, axis=0)
    shown = jnp.concatenate([best, jnp.zeros((ROWS - PER, LANES), F32)], axis=0).astype(BF16)
    groups = tall // ROWS
    for j in range(blocks):
        alive = place + j * (LANES // requests) < limit
        weight = jnp.where(alive, jnp.exp(scores[j] - high), 0.0)
        for i in range(groups):
            tile = weight[i * ROWS : (i + 1) * ROWS].astype(BF16)
            for c in range(peers):
                w_ref[c, j * groups + i] = tile
    for c in range(peers):
        w_ref[c, blocks * groups] = shown


def local_weights(parts, limit, requests, half_ctx):
    peers, tall, slim = parts.shape
    tiles = (tall // ROWS) * (slim // LANES) + 1
    return pl.pallas_call(
        lambda *refs: weight_kernel(requests, half_ctx, *refs),
        in_specs=[vmem()] * 2,
        out_specs=vmem(),
        out_shape=pltpu.VMEM((peers, tiles, ROWS, LANES), BF16),
        compiler_params=PARAMS,
        cost_estimate=AFTER_TRANSFER,
        name="weights",
    )(near(parts), near(limit))


def value_kernel(requests, w_ref, v_ref, out_ref):
    peers, tiles = w_ref.shape[:2]
    depth = v_ref.shape[1]
    slim = v_ref.shape[2] // peers // FOLD
    blocks = slim // LANES
    groups = (tiles - 1) // blocks
    used = requests * ROWS
    tops = [w_ref[c, tiles - 1].astype(F32) for c in range(peers)]
    best = tops[0]
    for c in range(1, peers):
        best = jnp.maximum(best, tops[c])
    which = iota((ROWS, slim), 1) % requests
    spare = jnp.zeros((ROWS - PER, slim), F32)
    ones = jnp.ones((depth, slim), BF16)
    acc = jnp.zeros((2 * depth, used), F32)
    for c in range(peers):
        fade = jnp.concatenate([jnp.exp(tops[c] - best)[0:PER]] * FOLD, axis=0)
        weight = jnp.concatenate(
            [
                jnp.concatenate([w_ref[c, j * groups + i].astype(F32) for i in range(groups)], axis=0) * fade
                for j in range(blocks)
            ],
            axis=1,
        )
        for k in range(FOLD):
            part = jnp.concatenate([weight[k * PER : (k + 1) * PER], spare], axis=0)
            masked = jnp.concatenate([jnp.where(which == r, part, 0.0) for r in range(requests)], axis=0)
            at = (c * FOLD + k) * slim
            values = jnp.concatenate([v_ref[1, :, at : at + slim], ones], axis=0)
            acc = acc + lax.dot_general(values, masked.astype(BF16), NT, preferred_element_type=F32)
    lane = iota((ROWS, LANES), 1)
    line = iota((ROWS, LANES), 0)
    mixed = jnp.where((lane // requests == line) & (lane < used), best, 0.0)
    row = jnp.broadcast_to(jnp.sum(mixed, axis=0, keepdims=True), (ROWS, LANES)).astype(BF16)
    a, b = iota((LANES, LANES), 0), iota((LANES, LANES), 1)
    moved = ((a // requests == b % ROWS) & (a % requests == b // ROWS)).astype(BF16)
    top = lax.dot_general(row, moved, NN, preferred_element_type=F32)
    out_ref[...] = jnp.zeros_like(out_ref)
    out_ref[0 : depth + ROWS, 0:used] = acc[0 : depth + ROWS]
    out_ref[depth : depth + ROWS, :] = jnp.where(line == 1, top, out_ref[depth : depth + ROWS, :])


def weighted_values(weights, kv_cache, requests):
    depth = kv_cache.shape[1]
    return pl.pallas_call(
        lambda *refs: value_kernel(requests, *refs),
        in_specs=[vmem()] * 2,
        out_specs=vmem(),
        out_shape=pltpu.VMEM((depth + ROWS, LANES), F32),
        compiler_params=PARAMS,
        cost_estimate=AFTER_TRANSFER,
        name="values",
    )(near(weights), near(kv_cache))


def merge_kernel(own_ref, left_ref, right_ref, out_ref):
    depth = own_ref.shape[0] - ROWS
    parts = (own_ref, left_ref, right_ref)
    highs = [p[depth + 1 : depth + 2, :] for p in parts]
    high = jnp.maximum(jnp.maximum(highs[0], highs[1]), highs[2])
    total = jnp.zeros((1, LANES), F32)
    summed = jnp.zeros((depth, LANES), F32)
    for part, top in zip(parts, highs):
        fade = jnp.exp(top - high)
        total = total + part[depth : depth + 1, :] * fade
        summed = summed + part[0:depth, :] * fade
    attn = summed / total
    held = jnp.zeros((ROWS, LANES), F32)
    for b in range(depth // ROWS):
        held = held + pltpu.roll(attn[b * ROWS : (b + 1) * ROWS], b * (LANES // HEADS), 1)
    held = held.astype(BF16)
    for k in range(out_ref.shape[0]):
        out_ref[k] = held


def merged(own, left, right, copies):
    return pl.pallas_call(
        merge_kernel,
        in_specs=[vmem()] * 3,
        out_specs=vmem(),
        out_shape=pltpu.VMEM((copies, ROWS, LANES), BF16),
        compiler_params=PARAMS,
        cost_estimate=AFTER_TRANSFER,
        name="merge",
    )(near(own), near(left), near(right))


def project_kernel(requests, attn_ref, w_ref, out_ref):
    width = w_ref.shape[0]
    heads = w_ref.shape[1] // (PER * HD)
    along = attn_ref.shape[0] // KVH
    blocks = HD // along // ROWS
    part = LANES // HEADS
    start = lax.axis_index(E) * (heads * along)
    pieces = [
        attn_ref[pl.ds(start + g * along, along)].astype(F32).reshape(along * ROWS, LANES) for g in range(heads)
    ]
    group = iota((along * ROWS, LANES), 1) // part
    stacked = []
    for b in range(blocks):
        mixed = jnp.zeros((along * ROWS, LANES), F32)
        for g in range(heads):
            mixed = jnp.where(group == g, pltpu.roll(pieces[g], ((g - b) * part) % LANES, 1), mixed)
        stacked.append(mixed)
    mixed = jnp.concatenate(stacked, axis=0).astype(BF16)
    d, k = iota((HD, HD), 0), iota((HD, HD), 1)
    order = (
        (d // (blocks * ROWS) == (k // ROWS) % along)
        & ((d // ROWS) % blocks == k // (along * ROWS))
        & (d % ROWS == k % ROWS)
    ).astype(BF16)
    attn = lax.dot_general(order, mixed, NN, preferred_element_type=F32).astype(BF16)
    lane = iota((width, LANES), 1)
    total = jnp.zeros((width, LANES), F32)
    for t in range(PER):
        for g in range(heads):
            at = g * PER * HD + t * HD
            term = lax.dot_general(w_ref[:, at : at + HD], attn, NN, preferred_element_type=F32)
            total = jnp.where((lane % ROWS == t) & (lane // part == g), term, total)
    place = iota((ROWS, LANES), 1)
    fold = ((place % part) // ROWS == iota((ROWS, LANES), 0)) & (place % ROWS < PER)
    folded = lax.dot_general(
        fold.astype(F32), total, NT, preferred_element_type=F32, precision=lax.Precision.HIGHEST
    )
    out_ref[...] = folded[0:requests, :]


def projected(attn, w_out, requests):
    return pl.pallas_call(
        lambda *refs: project_kernel(requests, *refs),
        in_specs=[vmem()] * 2,
        out_specs=vmem(),
        out_shape=pltpu.VMEM((requests, w_out.shape[1]), F32),
        compiler_params=PARAMS,
        cost_estimate=AFTER_TRANSFER,
        name="project",
    )(near(attn), near(w_out.T))


def attend_kernel(residual_ref, left_ref, right_ref, out_ref, copies_ref):
    attended = (residual_ref[...].astype(F32) + (left_ref[...] + right_ref[...])).astype(BF16)
    out_ref[...] = attended
    for k in range(copies_ref.shape[0]):
        copies_ref[k] = attended


def attend(residual, left, right, copies):
    return pl.pallas_call(
        attend_kernel,
        in_specs=[vmem()] * 3,
        out_specs=[vmem()] * 2,
        out_shape=[
            pltpu.VMEM(residual.shape, BF16),
            pltpu.VMEM((copies, *residual.shape), BF16),
        ],
        compiler_params=PARAMS,
        cost_estimate=AFTER_TRANSFER,
        name="attend",
    )(near(residual), near(left), near(right))


def expert_kernel(x_ref, gain_ref, router_ref, routing_ref, gate_ref, up_ref, down_ref, out_ref):
    requests = x_ref.shape[1]
    model = gain_ref.shape[0]
    held, _, hidden = gate_ref.shape
    experts_all = router_ref.shape[0]
    blocks, _, width = out_ref.shape
    widened = jnp.concatenate([x_ref[k].astype(F32) for k in range(blocks)], axis=1)
    mean_square = jnp.sum(widened * widened, axis=-1, keepdims=True) * (1.0 / model)
    normed = (widened * lax.rsqrt(mean_square + 1e-05) * gain_ref[...].astype(F32).reshape(1, model)).astype(BF16)
    row = iota((requests, experts_all), 0)
    column = iota((requests, experts_all), 1)
    exact = normed.astype(F32)
    logits = jnp.zeros((requests, experts_all), F32)
    for k in range(experts_all):
        logit = jnp.sum(exact * router_ref[k : k + 1, :].astype(F32), axis=-1, keepdims=True)
        logits = jnp.where(column == k, logit, logits)
    picked = []
    for k in range(2):
        chosen = jnp.full((requests, experts_all), routing_ref[k, 0], jnp.int32)
        for r in range(1, requests):
            chosen = jnp.where(row == r, routing_ref[k, r], chosen)
        picked.append(chosen == column)
    ahead = [jnp.sum(jnp.where(p, logits, 0.0), axis=-1, keepdims=True) for p in picked]
    first = jax.nn.sigmoid(ahead[0] - ahead[1])
    combine = jnp.where(picked[0], first, 0.0) + jnp.where(picked[1], 1.0 - first, 0.0)
    core = lax.axis_index(E)
    active = []
    for k in range(held):
        share = jnp.sum(jnp.where(column == core * held + k, combine, 0.0), axis=-1, keepdims=True)
        gate = lax.dot_general(normed, gate_ref[k], NN, preferred_element_type=F32)
        up = lax.dot_general(normed, up_ref[k], NN, preferred_element_type=F32)
        active.append((jax.nn.silu(gate) * up * share).astype(BF16))
    activation = jnp.concatenate(active, axis=-1)
    down = down_ref[...].reshape(held * hidden, model)
    terms = lax.dot_general(activation, down, NN, preferred_element_type=F32)
    for k in range(blocks):
        out_ref[k] = terms[:, k * width : (k + 1) * width]


def experts(gathered, norm_gain, router, routing, w_gate, w_up, w_down, seq_count):
    requests = gathered.shape[1]
    model = norm_gain.shape[0]
    return pl.pallas_call(
        expert_kernel,
        in_specs=[vmem()] * 3 + [pl.BlockSpec(memory_space=pltpu.SMEM)] + [vmem()] * 3,
        out_specs=vmem(),
        out_shape=pltpu.VMEM((seq_count, requests, model // seq_count), F32),
        compiler_params=PARAMS,
        name="experts",
    )(
        near(gathered),
        near(norm_gain),
        near(router.T),
        routing.T,
        near(w_gate),
        near(w_up),
        near(w_down),
    )


def on_device(
    residual,
    queries,
    new_entries,
    kv_cache,
    lengths,
    routing,
    w_out,
    norm_gain,
    router,
    w_gate,
    w_up,
    w_down,
):
    requests = lengths.shape[0]
    seq_count = lax.axis_size(SEQ)
    half_ctx = kv_cache.shape[2] // requests
    mine, limit = packed(queries, new_entries, lengths)
    scores, own = partial_scores(mine, swapped(mine), fetched_keys(kv_cache))
    weights = local_weights(to_everyone(scores, X), limit, requests, half_ctx)
    part = weighted_values(to_everyone(weights, X), kv_cache, requests)
    attn = merged(own, part, swapped(part), seq_count)
    head_terms = projected(to_everyone(attn, SEQ), w_out, requests)
    attended, copies = attend(residual, head_terms, swapped(head_terms), seq_count)
    gathered = to_everyone(copies, SEQ)
    blocks = experts(gathered, norm_gain, router, routing, w_gate, w_up, w_down, seq_count)
    reduced = to_everyone(blocks, SEQ).sum(axis=0)
    expert_out = (reduced + swapped(reduced)).astype(BF16)
    return (attended, expert_out)


def solution(mesh):
    along_x = mesh.shape["seq"] // KVH
    split = Mesh(
        mesh.devices.reshape(mesh.shape["groups"], KVH, along_x, mesh.shape["expert"]),
        ("groups", Y, X, E),
    )
    return jax.shard_map(
        on_device,
        mesh=split,
        in_specs=(
            P("groups", SEQ),
            P("groups", E),
            P(None, "groups", E),
            P(None, SEQ, ("groups", E)),
            P("groups"),
            P("groups", None),
            P(E, SEQ),
            P(),
            P(),
            P(E, None, SEQ),
            P(E, None, SEQ),
            P(E, SEQ, None),
        ),
        out_specs=(P("groups", SEQ), P("groups", SEQ)),
        check_vma=False,
    )
```

```python
import math

import jax
import jax.numpy as jnp
from jax import lax
from jax.experimental import pallas as pl
from jax.experimental.pallas import tpu as pltpu
from jax.sharding import Mesh
from jax.sharding import PartitionSpec as P

H = 48
KVH = 8
HD = 128
PER = H // KVH
Y = "seq_0"
X = "seq_1"
SEQ = (Y, X)
E = "expert"
LANES = 128
ROWS = 8
FOLD = 4
HEADS = 4
F32 = jnp.float32
BF16 = jnp.bfloat16
LOW = -1e30
LARGEST = 6.0
SCALE = 1.0 / math.sqrt(HD)
AFTER_TRANSFER = pl.CostEstimate(flops=20_000_000_000, transcendentals=0, bytes_accessed=1 << 24)
PARAMS = pltpu.CompilerParams(vmem_limit_bytes=16 << 20)
NT = (((1,), (1,)), ((), ()))
NN = (((1,), (0,)), ((), ()))


def iota(shape, dim):
    return lax.broadcasted_iota(jnp.int32, shape, dim)


def vmem():
    return pl.BlockSpec(memory_space=pltpu.VMEM)


def exponent_per_unit(depth):
    return 80.0 / (LARGEST * LARGEST * depth * SCALE)


def near(array):
    return pltpu.with_memory_space_constraint(array, pltpu.VMEM)


def far(array):
    return pltpu.with_memory_space_constraint(array, pltpu.HBM)


def swapped(shard):
    return lax.ppermute(shard, E, [(0, 1), (1, 0)])


def to_everyone(copies, axes):
    return lax.all_to_all(copies, axes, split_axis=0, concat_axis=0, tiled=True)


def pack_kernel(q_ref, new_ref, lengths_ref, packed_ref, limit_ref, sizes_ref, sems):
    requests = q_ref.shape[0]
    own_heads = q_ref.shape[1] // (PER * HD)
    local = lax.axis_index(Y) % own_heads
    span = PER * HD
    head = pl.ds(pl.multiple_of(local * HD, LANES), HD)
    copies = [
        pltpu.make_async_copy(lengths_ref, sizes_ref, sems.at[0]),
        pltpu.make_async_copy(
            q_ref.at[:, pl.ds(pl.multiple_of(local * span, LANES), span)], packed_ref.at[:, 0:span], sems.at[1]
        ),
    ]
    for i in range(2):
        copies.append(
            pltpu.make_async_copy(
                new_ref.at[i, :, head], packed_ref.at[:, span + i * HD : span + (i + 1) * HD], sems.at[2 + i]
            )
        )
    for copy in copies:
        copy.start()
    copies[0].wait()
    which = iota((ROWS, LANES), 1) % requests
    limit = jnp.full((ROWS, LANES), sizes_ref[0], jnp.int32)
    for r in range(1, requests):
        limit = jnp.where(which == r, sizes_ref[r], limit)
    limit_ref[...] = limit
    for copy in copies[1:]:
        copy.wait()


def packed(queries, new_entries, lengths):
    requests = queries.shape[0]
    return pl.pallas_call(
        pack_kernel,
        in_specs=[pl.BlockSpec(memory_space=pltpu.HBM)] * 3,
        out_specs=[vmem()] * 2,
        out_shape=[
            pltpu.VMEM((requests, PER * HD + 2 * HD), BF16),
            pltpu.VMEM((ROWS, LANES), jnp.int32),
        ],
        scratch_shapes=[pltpu.SMEM((requests,), jnp.int32), pltpu.SemaphoreType.DMA((4,))],
        compiler_params=PARAMS,
        name="pack",
    )(far(queries), far(new_entries), far(lengths))


def score_kernel(peers, own_heads, mine_ref, other_ref, k_ref, s_ref, own_ref, rows_ref):
    requests = mine_ref.shape[0]
    depth = k_ref.shape[0]
    width = k_ref.shape[1] // peers
    slim = width // FOLD
    x = lax.axis_index(X)
    mine = (lax.axis_index(Y) // own_heads) == lax.axis_index(E)
    q = jnp.where(mine, mine_ref[...].astype(F32), other_ref[...].astype(F32))
    rows_ref[...] = jnp.zeros_like(rows_ref)
    for r in range(requests):
        for t in range(PER):
            rows_ref[r * ROWS + t : r * ROWS + t + 1, :] = q[r : r + 1, t * HD : (t + 1) * HD]
    fresh = [q[:, (PER + i) * HD : (PER + i + 1) * HD].astype(BF16) for i in range(2)]

    rolled = pltpu.roll(rows_ref[0 : requests * ROWS, :], (HD - x * depth) % HD, 1)
    query = rolled[:, 0:depth].astype(BF16)
    which = iota((ROWS, slim), 1) % requests
    for c in range(peers):
        folds = []
        for k in range(FOLD):
            at = c * width + k * slim
            found = lax.dot_general(query, k_ref[:, at : at + slim], NN, preferred_element_type=F32)
            score = found[0:ROWS]
            for r in range(1, requests):
                score = jnp.where(which == r, found[r * ROWS : (r + 1) * ROWS], score)
            folds.append(score[0:PER])
        power = jnp.concatenate(folds, axis=0) * (SCALE * exponent_per_unit(depth))
        s_ref[c] = jnp.exp(power).astype(BF16)

    rows = rows_ref[...].astype(BF16)
    every = lax.dot_general(fresh[0], rows, NT, preferred_element_type=F32)
    own_row = iota(every.shape, 1) // ROWS == iota(every.shape, 0)
    score = jnp.sum(jnp.where(own_row, every, 0.0), axis=0, keepdims=True) * SCALE
    pick = (iota((depth, HD), 1) == iota((depth, HD), 0) + x * depth).astype(BF16)
    values = lax.dot_general(pick, fresh[1], NT, preferred_element_type=F32).astype(BF16)
    spread = (iota((requests, LANES), 1) // ROWS == iota((requests, LANES), 0)).astype(BF16)
    own_ref[0:depth, :] = lax.dot_general(values, spread, NN, preferred_element_type=F32)
    line = iota((ROWS, LANES), 0)
    own_ref[depth : depth + ROWS, :] = jnp.where(line == 0, 1.0, jnp.where(line == 1, score, 0.0))


def key_kernel(kv_ref, k_ref, sem):
    fetch = pltpu.make_async_copy(kv_ref.at[0], k_ref, sem)
    fetch.start()
    fetch.wait()


def fetched_keys(kv_cache):
    return pl.pallas_call(
        key_kernel,
        in_specs=[pl.BlockSpec(memory_space=pltpu.HBM)],
        out_specs=vmem(),
        out_shape=pltpu.VMEM(kv_cache.shape[1:], BF16),
        scratch_shapes=[pltpu.SemaphoreType.DMA],
        compiler_params=PARAMS,
        name="keys",
    )(far(kv_cache))


def partial_scores(mine, other, keys):
    depth = keys.shape[0]
    peers = lax.axis_size(X)
    own_heads = KVH // lax.axis_size(E)
    slim = keys.shape[1] // peers // FOLD
    return pl.pallas_call(
        lambda *refs: score_kernel(peers, own_heads, *refs),
        in_specs=[vmem()] * 3,
        out_specs=[vmem()] * 2,
        out_shape=[pltpu.VMEM((peers, FOLD * PER, slim), BF16), pltpu.VMEM((depth + ROWS, LANES), F32)],
        scratch_shapes=[pltpu.VMEM((LANES, HD), F32)],
        compiler_params=PARAMS,
        name="scores",
    )(near(mine), near(other), near(keys))


def weight_kernel(requests, half_ctx, parts_ref, limit_ref, w_ref):
    peers, tall, slim = parts_ref.shape
    blocks = slim // LANES
    start = lax.axis_index(E) * half_ctx + lax.axis_index(X) * (FOLD * slim // requests)
    limit = jnp.concatenate([limit_ref[...]] * (tall // ROWS), axis=0)
    place = iota((tall, LANES), 1) // requests + start + (iota((tall, LANES), 0) // PER) * (slim // requests)
    scores = []
    high = jnp.full((tall, LANES), LOW, F32)
    for j in range(blocks):
        at = slice(j * LANES, (j + 1) * LANES)
        total = jnp.log(parts_ref[0, :, at].astype(F32))
        for c in range(1, peers):
            total = total + jnp.log(parts_ref[c, :, at].astype(F32))
        alive = place + j * (LANES // requests) < limit
        total = jnp.where(alive, total * (1.0 / exponent_per_unit(HD // peers)), LOW)
        scores.append(total)
        high = jnp.maximum(high, total)
    best = high[0:PER]
    for k in range(1, FOLD):
        best = jnp.maximum(best, high[k * PER : (k + 1) * PER])
    step = requests
    while step < LANES:
        best = jnp.maximum(best, pltpu.roll(best, step, 1))
        step *= 2
    best16 = best.astype(BF16)
    best = best16.astype(F32)
    high = jnp.concatenate([best] * FOLD, axis=0)
    shown = jnp.concatenate([best, jnp.zeros((ROWS - PER, LANES), F32)], axis=0).astype(BF16)
    groups = tall // ROWS
    for j in range(blocks):
        alive = place + j * (LANES // requests) < limit
        weight = jnp.where(alive, jnp.exp(scores[j] - high), 0.0)
        for i in range(groups):
            tile = weight[i * ROWS : (i + 1) * ROWS].astype(BF16)
            for c in range(peers):
                w_ref[c, j * groups + i] = tile
    for c in range(peers):
        w_ref[c, blocks * groups] = shown


def local_weights(parts, limit, requests, half_ctx):
    peers, tall, slim = parts.shape
    tiles = (tall // ROWS) * (slim // LANES) + 1
    return pl.pallas_call(
        lambda *refs: weight_kernel(requests, half_ctx, *refs),
        in_specs=[vmem()] * 2,
        out_specs=vmem(),
        out_shape=pltpu.VMEM((peers, tiles, ROWS, LANES), BF16),
        compiler_params=PARAMS,
        cost_estimate=AFTER_TRANSFER,
        name="weights",
    )(near(parts), near(limit))


def value_kernel(requests, w_ref, v_ref, out_ref):
    peers, tiles = w_ref.shape[:2]
    depth = v_ref.shape[1]
    slim = v_ref.shape[2] // peers // FOLD
    blocks = slim // LANES
    groups = (tiles - 1) // blocks
    used = requests * ROWS
    tops = [w_ref[c, tiles - 1].astype(F32) for c in range(peers)]
    best = tops[0]
    for c in range(1, peers):
        best = jnp.maximum(best, tops[c])
    which = iota((ROWS, slim), 1) % requests
    spare = jnp.zeros((ROWS - PER, slim), F32)
    ones = jnp.ones((depth, slim), BF16)
    acc = jnp.zeros((2 * depth, used), F32)
    for c in range(peers):
        fade = jnp.concatenate([jnp.exp(tops[c] - best)[0:PER]] * FOLD, axis=0)
        weight = jnp.concatenate(
            [
                jnp.concatenate([w_ref[c, j * groups + i].astype(F32) for i in range(groups)], axis=0) * fade
                for j in range(blocks)
            ],
            axis=1,
        )
        for k in range(FOLD):
            part = jnp.concatenate([weight[k * PER : (k + 1) * PER], spare], axis=0)
            masked = jnp.concatenate([jnp.where(which == r, part, 0.0) for r in range(requests)], axis=0)
            at = (c * FOLD + k) * slim
            values = jnp.concatenate([v_ref[1, :, at : at + slim], ones], axis=0)
            acc = acc + lax.dot_general(values, masked.astype(BF16), NT, preferred_element_type=F32)
    lane = iota((ROWS, LANES), 1)
    line = iota((ROWS, LANES), 0)
    mixed = jnp.where((lane // requests == line) & (lane < used), best, 0.0)
    row = jnp.broadcast_to(jnp.sum(mixed, axis=0, keepdims=True), (ROWS, LANES)).astype(BF16)
    a, b = iota((LANES, LANES), 0), iota((LANES, LANES), 1)
    moved = ((a // requests == b % ROWS) & (a % requests == b // ROWS)).astype(BF16)
    top = lax.dot_general(row, moved, NN, preferred_element_type=F32)
    out_ref[...] = jnp.zeros_like(out_ref)
    out_ref[0 : depth + ROWS, 0:used] = acc[0 : depth + ROWS]
    out_ref[depth : depth + ROWS, :] = jnp.where(line == 1, top, out_ref[depth : depth + ROWS, :])


def weighted_values(weights, kv_cache, requests):
    depth = kv_cache.shape[1]
    return pl.pallas_call(
        lambda *refs: value_kernel(requests, *refs),
        in_specs=[vmem()] * 2,
        out_specs=vmem(),
        out_shape=pltpu.VMEM((depth + ROWS, LANES), F32),
        compiler_params=PARAMS,
        cost_estimate=AFTER_TRANSFER,
        name="values",
    )(near(weights), near(kv_cache))


def merge_kernel(own_ref, left_ref, right_ref, out_ref):
    depth = own_ref.shape[0] - ROWS
    parts = (own_ref, left_ref, right_ref)
    highs = [p[depth + 1 : depth + 2, :] for p in parts]
    high = jnp.maximum(jnp.maximum(highs[0], highs[1]), highs[2])
    total = jnp.zeros((1, LANES), F32)
    summed = jnp.zeros((depth, LANES), F32)
    for part, top in zip(parts, highs):
        fade = jnp.exp(top - high)
        total = total + part[depth : depth + 1, :] * fade
        summed = summed + part[0:depth, :] * fade
    attn = summed / total
    held = jnp.zeros((ROWS, LANES), F32)
    for b in range(depth // ROWS):
        held = held + pltpu.roll(attn[b * ROWS : (b + 1) * ROWS], b * (LANES // HEADS), 1)
    held = held.astype(BF16)
    for k in range(out_ref.shape[0]):
        out_ref[k] = held


def merged(own, left, right, copies):
    return pl.pallas_call(
        merge_kernel,
        in_specs=[vmem()] * 3,
        out_specs=vmem(),
        out_shape=pltpu.VMEM((copies, ROWS, LANES), BF16),
        compiler_params=PARAMS,
        cost_estimate=AFTER_TRANSFER,
        name="merge",
    )(near(own), near(left), near(right))


def project_kernel(requests, attn_ref, w_ref, out_ref):
    width = w_ref.shape[0]
    heads = w_ref.shape[1] // (PER * HD)
    along = attn_ref.shape[0] // KVH
    blocks = HD // along // ROWS
    part = LANES // HEADS
    start = lax.axis_index(E) * (heads * along)
    pieces = [
        attn_ref[pl.ds(start + g * along, along)].astype(F32).reshape(along * ROWS, LANES) for g in range(heads)
    ]
    group = iota((along * ROWS, LANES), 1) // part
    stacked = []
    for b in range(blocks):
        mixed = jnp.zeros((along * ROWS, LANES), F32)
        for g in range(heads):
            mixed = jnp.where(group == g, pltpu.roll(pieces[g], ((g - b) * part) % LANES, 1), mixed)
        stacked.append(mixed)
    mixed = jnp.concatenate(stacked, axis=0).astype(BF16)
    d, k = iota((HD, HD), 0), iota((HD, HD), 1)
    order = (
        (d // (blocks * ROWS) == (k // ROWS) % along)
        & ((d // ROWS) % blocks == k // (along * ROWS))
        & (d % ROWS == k % ROWS)
    ).astype(BF16)
    attn = lax.dot_general(order, mixed, NN, preferred_element_type=F32).astype(BF16)
    lane = iota((width, LANES), 1)
    total = jnp.zeros((width, LANES), F32)
    for t in range(PER):
        for g in range(heads):
            at = g * PER * HD + t * HD
            term = lax.dot_general(w_ref[:, at : at + HD], attn, NN, preferred_element_type=F32)
            total = jnp.where((lane % ROWS == t) & (lane // part == g), term, total)
    place = iota((ROWS, LANES), 1)
    fold = ((place % part) // ROWS == iota((ROWS, LANES), 0)) & (place % ROWS < PER)
    folded = lax.dot_general(
        fold.astype(F32), total, NT, preferred_element_type=F32, precision=lax.Precision.HIGHEST
    )
    out_ref[...] = folded[0:requests, :]


def projected(attn, w_out, requests):
    return pl.pallas_call(
        lambda *refs: project_kernel(requests, *refs),
        in_specs=[vmem()] * 2,
        out_specs=vmem(),
        out_shape=pltpu.VMEM((requests, w_out.shape[1]), F32),
        compiler_params=PARAMS,
        name="project",
    )(near(attn), near(w_out.T))


def attend_kernel(residual_ref, left_ref, right_ref, out_ref, copies_ref):
    attended = (residual_ref[...].astype(F32) + (left_ref[...] + right_ref[...])).astype(BF16)
    out_ref[...] = attended
    for k in range(copies_ref.shape[0]):
        copies_ref[k] = attended


def attend(residual, left, right, copies):
    return pl.pallas_call(
        attend_kernel,
        in_specs=[vmem()] * 3,
        out_specs=[vmem()] * 2,
        out_shape=[
            pltpu.VMEM(residual.shape, BF16),
            pltpu.VMEM((copies, *residual.shape), BF16),
        ],
        compiler_params=PARAMS,
        name="attend",
    )(near(residual), near(left), near(right))


def expert_kernel(x_ref, gain_ref, router_ref, routing_ref, gate_ref, up_ref, down_ref, out_ref):
    requests = x_ref.shape[1]
    model = gain_ref.shape[0]
    held, _, hidden = gate_ref.shape
    experts_all = router_ref.shape[0]
    blocks, _, width = out_ref.shape
    widened = jnp.concatenate([x_ref[k].astype(F32) for k in range(blocks)], axis=1)
    mean_square = jnp.sum(widened * widened, axis=-1, keepdims=True) * (1.0 / model)
    normed = (widened * lax.rsqrt(mean_square + 1e-05) * gain_ref[...].astype(F32).reshape(1, model)).astype(BF16)
    row = iota((requests, experts_all), 0)
    column = iota((requests, experts_all), 1)
    exact = normed.astype(F32)
    logits = jnp.zeros((requests, experts_all), F32)
    for k in range(experts_all):
        logit = jnp.sum(exact * router_ref[k : k + 1, :].astype(F32), axis=-1, keepdims=True)
        logits = jnp.where(column == k, logit, logits)
    picked = []
    for k in range(2):
        chosen = jnp.full((requests, experts_all), routing_ref[k, 0], jnp.int32)
        for r in range(1, requests):
            chosen = jnp.where(row == r, routing_ref[k, r], chosen)
        picked.append(chosen == column)
    ahead = [jnp.sum(jnp.where(p, logits, 0.0), axis=-1, keepdims=True) for p in picked]
    first = jax.nn.sigmoid(ahead[0] - ahead[1])
    combine = jnp.where(picked[0], first, 0.0) + jnp.where(picked[1], 1.0 - first, 0.0)
    core = lax.axis_index(E)
    active = []
    for k in range(held):
        share = jnp.sum(jnp.where(column == core * held + k, combine, 0.0), axis=-1, keepdims=True)
        gate = lax.dot_general(normed, gate_ref[k], NN, preferred_element_type=F32)
        up = lax.dot_general(normed, up_ref[k], NN, preferred_element_type=F32)
        active.append((jax.nn.silu(gate) * up * share).astype(BF16))
    activation = jnp.concatenate(active, axis=-1)
    down = down_ref[...].reshape(held * hidden, model)
    terms = lax.dot_general(activation, down, NN, preferred_element_type=F32)
    for k in range(blocks):
        out_ref[k] = terms[:, k * width : (k + 1) * width]


def experts(gathered, norm_gain, router, routing, w_gate, w_up, w_down, seq_count):
    requests = gathered.shape[1]
    model = norm_gain.shape[0]
    return pl.pallas_call(
        expert_kernel,
        in_specs=[vmem()] * 3 + [pl.BlockSpec(memory_space=pltpu.SMEM)] + [vmem()] * 3,
        out_specs=vmem(),
        out_shape=pltpu.VMEM((seq_count, requests, model // seq_count), F32),
        compiler_params=PARAMS,
        name="experts",
    )(
        near(gathered),
        near(norm_gain),
        near(router.T),
        routing.T,
        near(w_gate),
        near(w_up),
        near(w_down),
    )


def on_device(
    residual,
    queries,
    new_entries,
    kv_cache,
    lengths,
    routing,
    w_out,
    norm_gain,
    router,
    w_gate,
    w_up,
    w_down,
):
    requests = lengths.shape[0]
    seq_count = lax.axis_size(SEQ)
    half_ctx = kv_cache.shape[2] // requests
    mine, limit = packed(queries, new_entries, lengths)
    scores, own = partial_scores(mine, swapped(mine), fetched_keys(kv_cache))
    weights = local_weights(to_everyone(scores, X), limit, requests, half_ctx)
    part = weighted_values(to_everyone(weights, X), kv_cache, requests)
    attn = merged(own, part, swapped(part), seq_count)
    head_terms = projected(to_everyone(attn, SEQ), w_out, requests)
    attended, copies = attend(residual, head_terms, swapped(head_terms), seq_count)
    gathered = to_everyone(copies, SEQ)
    blocks = experts(gathered, norm_gain, router, routing, w_gate, w_up, w_down, seq_count)
    reduced = to_everyone(blocks, SEQ).sum(axis=0)
    expert_out = (reduced + swapped(reduced)).astype(BF16)
    return (attended, expert_out)


def solution(mesh):
    along_x = mesh.shape["seq"] // KVH
    split = Mesh(
        mesh.devices.reshape(mesh.shape["groups"], KVH, along_x, mesh.shape["expert"]),
        ("groups", Y, X, E),
    )
    return jax.shard_map(
        on_device,
        mesh=split,
        in_specs=(
            P("groups", SEQ),
            P("groups", E),
            P(None, "groups", E),
            P(None, SEQ, ("groups", E)),
            P("groups"),
            P("groups", None),
            P(E, SEQ),
            P(),
            P(),
            P(E, None, SEQ),
            P(E, None, SEQ),
            P(E, SEQ, None),
        ),
        out_specs=(P("groups", SEQ), P("groups", SEQ)),
        check_vma=False,
    )
```
